32 devices in a mesh: grp: 8 (over z, x), tbl: 4 (over y, core).
Axes of the slice: x: 2, y: 2, z: 4, core: 2. Of those that a mesh axis runs over, the one named last changes fastest.
Arguments:
- next_ids: int32 [4096, 224], P(('grp', 'tbl')), may hold values from 0 to 6143
- next_lengths: int32 [4096, 26], P(('grp', 'tbl')), may hold values from 1 to 8
- slot_of_table: int32 [26], replicated, may hold values from 0 to 27, as said below
- tables: bfloat16 [28, 6144, 128], P('tbl'), may hold values from -2.5 to 2.5
- cross_input: bfloat16 [4096, 3456], P(('grp', 'tbl')), may hold values from -6 to 6
- cotangent: bfloat16 [4096, 3456], P(('grp', 'tbl')), may hold values from -6 to 6
- up_weight: bfloat16 [256, 3456], replicated, may hold values from -0.375 to 0.375
- down_weight: bfloat16 [3456, 256], replicated, may hold values from -0.109375 to 0.109375
Outputs:
- next_embedded: bfloat16 [4096, 3328], P(('grp', 'tbl'))
- grad_up: float32 [256, 3456], P('tbl', 'grp')
- grad_down: float32 [3456, 256], P('grp', 'tbl')
The draws below stay inside these ranges and needn't reach their ends.
Inputs may be any that keep to these rules, and one draw needn't show every extreme that they name: `next_ids`: entry 8 * s + k of an example's row is the k-th id of the bag held in slot s; entries with k at or past the bag's length, and all entries of slots that hold no table, are padding. `slot_of_table`: distinct slots; owner o along tbl holds slots o * 7 to o * 7 + 6, so an owner holds up to 7 tables and some owner holds exactly 7.
All inputs are finite; a program needn't handle non-finite values.
Results may differ from the reference program's by a relative error of at most 0.0049.
Values may be sent and summed in bfloat16 or wider, within the bound.
No kernel may reach another device: no remote copies, remote signals or barrier semaphores. Data moves between devices by JAX's collectives and lax.ppermute only.
A program may use at most 128 MiB of HBM per device.

```python
import math
import jax
import jax.numpy as jnp
import numpy as np
from jax import lax

F = 26
E = 128
R = 256
MAXLEN = 8
ROWS = 6144
B_DEV = 128
D = 3456
TOKENS = 4096
SLOTS_ALL = 28
N_TBL = 4


def draw_slot_of_table(key, part):
    return jax.random.permutation(key, SLOTS_ALL)[:F].astype(jnp.int32)


def plant(entries, stream_key, smallest, top_value):
    shape = entries.shape
    place = [jax.random.randint(jax.random.fold_in(stream_key, axis), (), 0, shape[axis]) for axis in range(len(shape))]
    entries = entries.at[tuple(place)].set(smallest)
    longest = shape.index(max(shape))
    place[longest] = (place[longest] + 1) % shape[longest]
    return entries.at[tuple(place)].set(top_value)


def block_scale(stream_key, shape, split, low, largest):
    loudness, own = 1.0, jax.random.fold_in(stream_key, 6)
    for dim, shards_of in split:
        heights = jnp.exp(jax.random.uniform(jax.random.fold_in(own, dim), (shards_of,), jnp.float32, low / len(split), largest / len(split)))
        loudness = loudness * jnp.repeat(heights, shape[dim] // shards_of).reshape([-1 if axis == dim else 1 for axis in range(len(shape))])
    return loudness


def cumulative_ranks(amount, slope):
    loads = [(1 << 20) // math.isqrt(standing ** slope) + 1 for standing in range(1, amount + 1)]
    deviation = 1 + sum(loads) // (1 << 30)
    return np.cumsum(np.array([max(1, weight // deviation) for weight in loads]))


def ranked_ids(key, extent, number_of, lean):
    table = cumulative_ranks(number_of, lean)
    pick = jax.random.randint(jax.random.fold_in(key, 1), extent, 0, int(table[number_of - 1]))
    grade = jnp.searchsorted(jnp.asarray(table, jnp.int32), pick, side="right")
    return jax.random.permutation(jax.random.fold_in(key, 2), number_of)[grade].astype(jnp.int32)


def gaussian(rng, extent, width, most, cuts=(), kind=jnp.bfloat16):
    entries = jax.random.normal(rng, extent, jnp.float32) * width
    if len(cuts) > 0:
        entries = block_scale(rng, extent, cuts, -0.22, 0.18) * entries
    return jnp.clip(entries, min=-most, max=most).astype(kind)


def setup_inputs(seed: int = 0) -> dict:
    key_list = jax.random.split(jax.random.key(seed), 9)
    return {
        "next_ids": plant(ranked_ids(key_list[0], (TOKENS, SLOTS_ALL * MAXLEN), ROWS, 2), jax.random.fold_in(key_list[0], 3), 0, ROWS - 1).astype(jnp.int32),
        "next_lengths": plant(jax.random.randint(key_list[1], (TOKENS, F), 1, MAXLEN + 1), jax.random.fold_in(key_list[1], 1), 1, MAXLEN).astype(jnp.int32),
        "slot_of_table": draw_slot_of_table(jax.random.fold_in(key_list[8], 71), 0),
        "tables": gaussian(key_list[3], (SLOTS_ALL, ROWS, E), 0.35, 2.5, ((0, 4),)),
        "cross_input": gaussian(key_list[4], (TOKENS, D), 1.0, 6.0, ((0, 32),)),
        "cotangent": gaussian(key_list[5], (TOKENS, D), 1.0, 6.0, ((0, 32),)),
        "up_weight": gaussian(key_list[6], (R, D), R ** -0.5, 0.375),
        "down_weight": gaussian(key_list[7], (D, R), D ** -0.5, 0.109375),
    }


def pool_block(tables, slot_of_table, ids, lengths):
    count = ids.shape[0]
    ids_three = ids.reshape(count, SLOTS_ALL, MAXLEN)
    chosen = jnp.take(ids_three, slot_of_table, axis=1)
    flat_table = tables.reshape(SLOTS_ALL * ROWS, E)
    index = (chosen + (slot_of_table * ROWS)[None, :, None]).astype(jnp.int32)
    picked = jnp.take(flat_table, index.reshape(-1), axis=0).reshape(count, F, MAXLEN, E)
    keep = lax.broadcasted_iota(jnp.int32, (count, F, MAXLEN), 2) < lengths[:, :, None]
    masked = jnp.where(keep[..., None], picked, jnp.zeros((), picked.dtype))
    pooled = lax.optimization_barrier(jnp.sum(masked.astype(jnp.float32), axis=2))
    return pooled.astype(jnp.bfloat16).reshape(count, F * E)

def reference(next_ids, next_lengths, slot_of_table, tables, cross_input, cotangent, up_weight, down_weight):
    blocks = TOKENS // B_DEV
    id_blocks = next_ids.reshape(blocks, B_DEV, SLOTS_ALL * MAXLEN)
    len_blocks = next_lengths.reshape(blocks, B_DEV, F)
    pooled = lax.map(lambda pair: pool_block(tables, slot_of_table, pair[0], pair[1]), (id_blocks, len_blocks))
    next_embedded = pooled.reshape(TOKENS, F * E)
    span = B_DEV * N_TBL
    input_blocks = cross_input.reshape(TOKENS // span, span, D)
    grad_blocks = cotangent.reshape(TOKENS // span, span, D)

    def step(carry, pair):
        total_up, total_down = carry
        inputs, grads = pair
        low = jnp.dot(inputs, down_weight, preferred_element_type=jnp.float32).astype(jnp.bfloat16)
        dz = (grads.astype(jnp.float32) * inputs.astype(jnp.float32)).astype(jnp.bfloat16)
        dlow = jnp.dot(dz, up_weight.T, preferred_element_type=jnp.float32).astype(jnp.bfloat16)
        total_up = total_up + jnp.dot(low.T, dz, preferred_element_type=jnp.float32)
        total_down = total_down + jnp.dot(inputs.T, dlow, preferred_element_type=jnp.float32)
        return ((total_up, total_down), None)
    start = (jnp.zeros((R, D), jnp.float32), jnp.zeros((D, R), jnp.float32))
    (total_up, total_down), unused = lax.scan(step, start, (input_blocks, grad_blocks))
    factor = 1.0 / math.sqrt(TOKENS)
    return (next_embedded, total_up * factor, total_down * factor)
```

```python
import functools
import math

import jax
import jax.numpy as jnp
from jax import lax
from jax.experimental import pallas as pl
from jax.experimental.pallas import tpu as pltpu
from jax.sharding import PartitionSpec as P

F32 = jnp.float32
BF16 = jnp.bfloat16
LANES = 128


def whole(memory=pltpu.VMEM):
    return pl.BlockSpec(memory_space=memory)


def mask_ids_kernel(slot_ref, ids_ref, lens_ref, out_ref, *, maxlen, rows):
    entries, batch = out_ref.shape
    feats = lens_ref.shape[1]
    slot_of_row = lax.broadcasted_iota(jnp.int32, (entries, feats), 0) // maxlen
    hit = (slot_of_row == slot_ref[...]).astype(F32)
    lens = lax.dot_general(
        hit, lens_ref[...].astype(F32), (((1,), (1,)), ((), ())), preferred_element_type=F32
    )
    place = lax.broadcasted_iota(jnp.int32, (entries, batch), 0) % maxlen
    keep = place.astype(F32) + 0.5 < lens
    out_ref[...] = jnp.where(keep, ids_ref[...].T, rows)


def mask_ids(slot_of_table, ids, lengths, maxlen, rows):
    return pl.pallas_call(
        functools.partial(mask_ids_kernel, maxlen=maxlen, rows=rows),
        in_specs=[whole()] * 3,
        out_specs=whole(),
        out_shape=jax.ShapeDtypeStruct((ids.shape[1], ids.shape[0]), jnp.int32),
        name="mask_ids",
    )(slot_of_table.reshape(1, -1), ids, lengths)


def pool_kernel(ids_ref, table_ref, out_ref, wide_ref, sum_ref, *, rows, chunk):
    groups, maxlen, batch = ids_ref.shape

    def widen(i, carry):
        start = pl.multiple_of(i * chunk, chunk)
        wide_ref[pl.ds(start, chunk), :] = table_ref[0, pl.ds(start, chunk), :].astype(F32)
        return carry

    lax.fori_loop(0, rows // chunk, widen, 0)
    wide_ref[pl.ds(rows, 8), :] = jnp.zeros((8, wide_ref.shape[1]), F32)

    def pool(g, carry):
        for b in range(batch):
            total = wide_ref[pl.ds(ids_ref[g, 0, b], 1), :]
            for k in range(1, maxlen):
                total = total + wide_ref[pl.ds(ids_ref[g, k, b], 1), :]
            sum_ref[pl.ds(b, 1), :] = total
        out_ref[g, 0] = sum_ref[...].astype(BF16)
        return carry

    lax.fori_loop(0, groups, pool, 0)


def pool_slots(ids, tables, first, count, maxlen):
    groups, entries, batch = ids.shape
    rows, width = tables.shape[1:]
    chunk = math.gcd(rows, 512)
    return pl.pallas_call(
        functools.partial(pool_kernel, rows=rows, chunk=chunk),
        grid=(count,),
        in_specs=[
            pl.BlockSpec(
                (groups, maxlen, batch), lambda s: (0, s + first, 0), memory_space=pltpu.SMEM
            ),
            pl.BlockSpec((1, rows, width), lambda s: (s + first, 0, 0)),
        ],
        out_specs=pl.BlockSpec((groups, 1, batch, width), lambda s: (0, s, 0, 0)),
        out_shape=jax.ShapeDtypeStruct((groups, count, batch, width), BF16),
        scratch_shapes=[pltpu.VMEM((rows + 8, width), F32), pltpu.VMEM((batch, width), F32)],
        name="pool_slots",
    )(ids, tables)


def place_kernel(slot_ref, *refs, slots, firsts, counts):
    parts, out_ref = refs[:-1], refs[-1]
    width = parts[0].shape[3]
    for f in range(slot_ref.shape[0]):
        slot = slot_ref[f]
        owner = slot // slots
        local = slot - owner * slots
        for part, first, count in zip(parts, firsts, counts):

            def put(part=part, first=first, f=f):
                out_ref[:, f * width : (f + 1) * width] = part[owner, local - first]

            if len(parts) == 1:
                put()
            else:
                pl.when((local >= first) & (local < first + count))(put)


def place(slot_of_table, parts, firsts, counts, slots):
    batch, width = parts[0].shape[2:]
    feats = slot_of_table.shape[0]
    return pl.pallas_call(
        functools.partial(place_kernel, slots=slots, firsts=firsts, counts=counts),
        in_specs=[whole(pltpu.SMEM)] + [whole()] * len(parts),
        out_specs=whole(),
        out_shape=jax.ShapeDtypeStruct((batch, feats * width), BF16),
        name="place",
    )(slot_of_table, *parts)


def grads_kernel(
    pos_ref, x_ref, ct_ref, xs_ref, cts_ref, down_ref, up_ref, *refs, owners, groups, rows_a
):
    tall = owners // 2
    far = groups // 2
    qa, qb = refs[:tall], refs[tall : tall + 2]
    both_ref, sum_ref = refs[tall + 2 :]
    core, y, x, z = pos_ref[0], pos_ref[1], pos_ref[2], pos_ref[3]
    batch, wide = x_ref.shape
    rank = down_ref.shape[1]
    part = rank // owners
    pair = 2 * batch
    for at, (a_ref, b_ref) in enumerate(((x_ref, ct_ref), (xs_ref, cts_ref))):
        a = a_ref[...]
        both_ref[pl.ds(at * batch, batch), :] = (b_ref[...].astype(F32) * a.astype(F32)).astype(BF16)
        both_ref[pl.ds(pair + at * batch, batch), :] = a
    low = jnp.dot(both_ref[pl.ds(pair, pair), :], down_ref[...], preferred_element_type=F32)
    dlow = lax.dot_general(
        both_ref[pl.ds(0, pair), :],
        up_ref[...],
        (((1,), (1,)), ((), ())),
        preferred_element_type=F32,
    )
    none = jnp.zeros((pair, part), F32)
    columns = []
    for ry in range(tall):
        owner = 2 * lax.rem(y + ry, tall) + core
        lo, dl = none, none
        for t in range(owners):
            lo = jnp.where(owner == t, low[:, t * part : (t + 1) * part], lo)
            dl = jnp.where(owner == t, dlow[:, t * part : (t + 1) * part], dl)
        columns.append(
            jnp.concatenate(
                [jnp.concatenate([lo, none], axis=1), jnp.concatenate([none, dl], axis=1)], axis=0
            )
        )
    right = jnp.concatenate(columns, axis=1).astype(BF16)
    step = 384 if wide % 384 == 0 else wide
    for d in range(0, wide, step):
        sum_ref[pl.ds(d, step), :] = lax.dot_general(
            both_ref[:, d : d + step], right, (((0,), (0,)), ((), ())), preferred_element_type=F32
        )
    each = wide // groups
    rows_b = each - rows_a
    block = 2 * part
    for rx in range(2):
        for r in range(far):
            g = 2 * lax.rem(z + r, far) + (x + rx - 2 * x * rx)
            start = pl.multiple_of(g * each, 16)
            for ry in range(tall):
                cols = slice(ry * block, (ry + 1) * block)
                qa[ry][rx, r] = sum_ref[pl.ds(start, rows_a), cols].astype(qa[ry].dtype)
                qb[rx][ry, r] = sum_ref[pl.ds(start + rows_a, rows_b), cols].astype(qb[rx].dtype)


def part_grads(pos, x, ct, xs, cts, down, up, owners, groups, rows_a):
    wide, rank = down.shape
    batch = x.shape[0]
    tall, far = owners // 2, groups // 2
    rows_b = wide // groups - rows_a
    block = 2 * (rank // owners)
    shape = jax.ShapeDtypeStruct
    qa = [shape((2, far, rows_a, block), F32 if ry == 0 else BF16) for ry in range(tall)]
    qb = [shape((tall, far, rows_b, block), F32 if rx == 0 else BF16) for rx in range(2)]
    out = pl.pallas_call(
        functools.partial(grads_kernel, owners=owners, groups=groups, rows_a=rows_a),
        in_specs=[whole(pltpu.SMEM)] + [whole()] * 6,
        out_specs=[whole()] * (tall + 2),
        out_shape=qa + qb,
        scratch_shapes=[
            pltpu.VMEM((4 * batch, wide), BF16),
            pltpu.VMEM((wide, tall * block), F32),
        ],
        name="part_grads",
    )(pos, x, ct, xs, cts, down, up)
    return out[:tall], out[tall:]


def fold_kernel(*refs, tall):
    ka, kb, ra, rb = refs[0], refs[1], refs[2 : tall + 1], refs[tall + 1]
    outs = refs[tall + 2 :]
    a_keep, a_send, b_keep, b_send = outs[0], outs[1], outs[2], outs[3:]

    def at_a(i):
        total = ka[i]
        for r in ra:
            total = total + r[i].astype(F32)
        return total

    def at_b(i):
        return kb[i] + rb[i].astype(F32)

    a_keep[...] = at_a(0)
    a_send[...] = at_a(1).astype(BF16)
    b_keep[...] = at_b(0)
    for ry in range(1, tall):
        b_send[ry - 1][...] = at_b(ry).astype(BF16)


def fold(ka, kb, ra, rb, tall):
    shape = jax.ShapeDtypeStruct
    a, b = ka.shape[1:], kb.shape[1:]
    out = [shape(a, F32), shape(a, BF16), shape(b, F32)] + [shape(b, BF16)] * (tall - 1)
    res = pl.pallas_call(
        functools.partial(fold_kernel, tall=tall),
        in_specs=[whole()] * (tall + 2),
        out_specs=[whole()] * len(out),
        out_shape=out,
        name="fold",
    )(ka, kb, *ra, rb)
    return res[0], res[1], res[2], res[3:]


def join_kernel(*refs, tall, far):
    ka, kb, ra, rb, outs = refs[0], refs[1], refs[2], refs[3 : tall + 2], refs[tall + 2 :]
    rows_a = ka.shape[1]
    for r in range(far):
        sa = ka[r] + ra[r].astype(F32)
        sb = kb[r]
        for one in rb:
            sb = sb + one[r].astype(F32)
        outs[r][0:rows_a, :] = sa.astype(outs[r].dtype)
        outs[r][rows_a:, :] = sb.astype(outs[r].dtype)


def join(ka, kb, ra, rb, tall, far):
    rows, block = ka.shape[1] + kb.shape[1], ka.shape[2]
    out = [jax.ShapeDtypeStruct((rows, block), F32 if r == 0 else BF16) for r in range(far)]
    return pl.pallas_call(
        functools.partial(join_kernel, tall=tall, far=far),
        in_specs=[whole()] * (tall + 2),
        out_specs=[whole()] * far,
        out_shape=out,
        name="join",
    )(ka, kb, ra, *rb)


def finish_kernel(*refs, factor):
    up_ref, down_ref = refs[-2:]
    total = refs[0][...]
    for r in refs[1:-2]:
        total = total + r[...].astype(F32)
    total = total * factor
    half = total.shape[1] // 2
    up_ref[...] = total.T[:half, :]
    down_ref[...] = total[:, half:]


def finish(keep, came, factor):
    rows, block = keep.shape
    half = block // 2
    shape = jax.ShapeDtypeStruct
    return pl.pallas_call(
        functools.partial(finish_kernel, factor=factor),
        in_specs=[whole()] * (1 + len(came)),
        out_specs=[whole()] * 2,
        out_shape=[shape((half, rows), F32), shape((rows, half), F32)],
        name="finish",
    )(keep, *came)


def grads_by_exchange(x, ct, up, down, factor):
    owners, groups = lax.axis_size("tbl"), lax.axis_size("grp")
    tall, far = owners // 2, groups // 2
    t, g = lax.axis_index("tbl"), lax.axis_index("grp")
    pos = jnp.stack([t % 2, t // 2, g % 2, g // 2]).astype(jnp.int32)
    other_core = [(i, i ^ 1) for i in range(owners)]
    other_x = [(i, i ^ 1) for i in range(groups)]

    def to_y(ry):
        return [(i, 2 * ((i // 2 + ry) % tall) + i % 2) for i in range(owners)]

    def to_z(r):
        return [(i, 2 * ((i // 2 + r) % far) + i % 2) for i in range(groups)]

    xs = lax.ppermute(x, "tbl", other_core)
    cts = lax.ppermute(ct, "tbl", other_core)
    rows_a = (x.shape[1] // groups // 2) // 16 * 16
    qa, qb = part_grads(pos, x, ct, xs, cts, down, up, owners, groups, rows_a)
    ra = [lax.ppermute(qa[ry], "tbl", to_y(ry)) for ry in range(1, tall)]
    rb = lax.ppermute(qb[1], "grp", other_x)
    ka, sa, kb, sb = fold(qa[0], qb[0], ra, rb, tall)
    ra = lax.ppermute(sa, "grp", other_x)
    rb = [lax.ppermute(s, "tbl", to_y(ry + 1)) for ry, s in enumerate(sb)]
    out = join(ka, kb, ra, rb, tall, far)
    came = [lax.ppermute(out[r], "grp", to_z(r)) for r in range(1, far)]
    return finish(out[0], came, factor)


def grads_plain(x, ct, up, down, factor):
    low = jnp.dot(x, down, preferred_element_type=F32).astype(BF16)
    dz = (ct.astype(F32) * x.astype(F32)).astype(BF16)
    dlow = jnp.dot(dz, up.T, preferred_element_type=F32).astype(BF16)
    part_up = jnp.dot(low.T, dz, preferred_element_type=F32) * factor
    part_down = jnp.dot(x.T, dlow, preferred_element_type=F32) * factor
    owner_up = lax.psum_scatter(part_up, "tbl", scatter_dimension=0, tiled=True)
    owner_down = lax.psum_scatter(part_down, "tbl", scatter_dimension=1, tiled=True)
    return (
        lax.psum_scatter(owner_up, "grp", scatter_dimension=1, tiled=True),
        lax.psum_scatter(owner_down, "grp", scatter_dimension=0, tiled=True),
    )


def on_device(ids, lengths, slot_of_table, tables, x, ct, up, down):
    owners, groups = lax.axis_size("tbl"), lax.axis_size("grp")
    batch = ids.shape[0]
    slots, rows = tables.shape[:2]
    maxlen = ids.shape[1] // (slots * owners)
    factor = 1.0 / math.sqrt(batch * owners * groups)

    masked = mask_ids(slot_of_table, ids, lengths, maxlen, rows)
    got = lax.all_to_all(masked.reshape(owners, slots * maxlen, batch), "tbl", 0, 0)

    each, part = x.shape[1] // groups, down.shape[1] // owners
    tiled = owners % 2 == 0 and groups % 2 == 0 and each % 16 == 0 and 2 * part % LANES == 0
    grads = grads_by_exchange if tiled else grads_plain
    grad_up, grad_down = grads(x, ct, up, down, factor)

    cut = (slots + 1) // 2
    firsts, counts = (0, cut), (cut, slots - cut)
    parts = [
        lax.all_to_all(pool_slots(got, tables, first, count, maxlen), "tbl", 0, 0)
        for first, count in zip(firsts, counts)
    ]
    embedded = place(slot_of_table, parts, firsts, counts, slots)
    return embedded, grad_up, grad_down


def solution(mesh):
    rows = P(("grp", "tbl"), None)
    return jax.shard_map(
        on_device,
        mesh=mesh,
        in_specs=(rows, rows, P(), P("tbl", None, None), rows, rows, P(), P()),
        out_specs=(rows, P("tbl", "grp"), P("grp", "tbl")),
        check_vma=False,
    )
```

```python
import functools
import math

import jax
import jax.numpy as jnp
from jax import lax
from jax.experimental import pallas as pl
from jax.experimental.pallas import tpu as pltpu
from jax.sharding import PartitionSpec as P


F32 = jnp.float32
BF16 = jnp.bfloat16
LANES = 128


def room(mebibytes):
    return pltpu.CompilerParams(vmem_limit_bytes=mebibytes * 2**20)


def whole(memory=pltpu.VMEM):
    return pl.BlockSpec(memory_space=memory)


def in_hbm(x):
    return pltpu.with_memory_space_constraint(x, pltpu.HBM)


def mask_ids_kernel(slot_ref, ids_ref, lens_ref, out_ref, *, maxlen, rows):
    entries, batch = out_ref.shape
    feats = lens_ref.shape[0]
    slot_of_row = lax.broadcasted_iota(jnp.int32, (entries, feats), 0) // maxlen
    hit = (slot_of_row == slot_ref[...]).astype(F32)
    lens = jnp.dot(hit, lens_ref[...].astype(F32), preferred_element_type=F32)
    place = lax.broadcasted_iota(jnp.int32, (entries, batch), 0) % maxlen
    keep = place.astype(F32) + 0.5 < lens
    out_ref[...] = jnp.where(keep, ids_ref[...], rows)


def mask_ids(slot_of_table, ids, lengths, maxlen, rows):
    return pl.pallas_call(
        functools.partial(mask_ids_kernel, maxlen=maxlen, rows=rows),
        in_specs=[whole()] * 3,
        out_specs=whole(),
        out_shape=jax.ShapeDtypeStruct((ids.shape[1], ids.shape[0]), jnp.int32),
        compiler_params=room(4),
        name="mask_ids",
    )(slot_of_table.reshape(1, -1), ids.T, lengths.T)


def pool_kernel(ids_ref, table_ref, out_ref, wide_ref, sum_ref, *rest, first, chunk):
    rows, width = table_ref.shape[1:]
    groups, _, batch, _ = out_ref.shape
    near, sem = rest[:groups], rest[groups]
    maxlen = near[0].shape[0]
    step, steps = pl.program_id(0), pl.num_programs(0)

    def fetch(g, at):
        start = pl.multiple_of((first + at) * maxlen, maxlen)
        return pltpu.make_async_copy(ids_ref.at[g, pl.ds(start, maxlen)], near[g], sem.at[g])

    @pl.when(step == 0)
    def _():
        for g in range(groups):
            fetch(g, 0).start()

    def widen(i, carry):
        start = pl.multiple_of(i * chunk, chunk)
        wide_ref[pl.ds(start, chunk), :] = table_ref[0, pl.ds(start, chunk), :].astype(F32)
        return carry

    lax.fori_loop(0, rows // chunk, widen, 0)
    wide_ref[pl.ds(rows, 8), :] = jnp.zeros((8, width), F32)
    for g in range(groups):
        fetch(g, step).wait()
        for b in range(batch):
            total = wide_ref[pl.ds(near[g][0, b], 1), :]
            for k in range(1, maxlen):
                total = total + wide_ref[pl.ds(near[g][k, b], 1), :]
            sum_ref[pl.ds(b, 1), :] = total
        out_ref[g, 0] = sum_ref[...].astype(BF16)

        @pl.when(step + 1 < steps)
        def _(g=g):
            fetch(g, step + 1).start()


def pool_slots(ids, tables, first, count, maxlen):
    groups, _, batch = ids.shape
    rows, width = tables.shape[1:]
    return pl.pallas_call(
        functools.partial(pool_kernel, first=first, chunk=math.gcd(rows, 512)),
        grid=(count,),
        in_specs=[
            pl.BlockSpec(memory_space=pl.ANY),
            pl.BlockSpec((1, rows, width), lambda s: (s + first, 0, 0)),
        ],
        out_specs=pl.BlockSpec((groups, 1, batch, width), lambda s: (0, s, 0, 0)),
        out_shape=jax.ShapeDtypeStruct((groups, count, batch, width), BF16),
        scratch_shapes=[pltpu.VMEM((rows + 8, width), F32), pltpu.VMEM((batch, width), F32)]
        + [pltpu.SMEM((maxlen, batch), jnp.int32)] * groups
        + [pltpu.SemaphoreType.DMA((groups,))],
        compiler_params=room(12),
        name="pool_slots",
    )(ids, in_hbm(tables))


def place_kernel(slot_ref, *refs, slots, firsts, counts):
    parts, out_ref = refs[:-1], refs[-1]
    width = parts[0].shape[3]
    for f in range(slot_ref.shape[0]):
        slot = slot_ref[f]
        owner = slot // slots
        local = slot - owner * slots
        for part, first, count in zip(parts, firsts, counts):

            def put(part=part, first=first, f=f):
                out_ref[:, f * width : (f + 1) * width] = part[owner, local - first]

            if len(parts) == 1:
                put()
            else:
                pl.when((local >= first) & (local < first + count))(put)


def place(slot_of_table, parts, firsts, counts, slots):
    batch, width = parts[0].shape[2:]
    feats = slot_of_table.shape[0]
    return pl.pallas_call(
        functools.partial(place_kernel, slots=slots, firsts=firsts, counts=counts),
        in_specs=[whole(pltpu.SMEM)] + [whole()] * len(parts),
        out_specs=whole(),
        out_shape=jax.ShapeDtypeStruct((batch, feats * width), BF16),
        compiler_params=room(8),
        name="place",
    )(slot_of_table, *parts)


def grads_kernel(pos_ref, x_ref, ct_ref, xs_ref, cts_ref, down_ref, up_ref, *refs, owners, groups):
    tall, far = owners // 2, groups // 2
    outs = refs[: 2 * tall]
    both_ref, sum_ref = refs[2 * tall :]
    core, y, x, z = pos_ref[0], pos_ref[1], pos_ref[2], pos_ref[3]
    batch, wide = x_ref.shape
    rank = down_ref.shape[1]
    part = rank // owners
    pair = 2 * batch
    for at, (a_ref, b_ref) in enumerate(((x_ref, ct_ref), (xs_ref, cts_ref))):
        a = a_ref[...]
        both_ref[pl.ds(at * batch, batch), :] = (b_ref[...].astype(F32) * a.astype(F32)).astype(BF16)
        both_ref[pl.ds(pair + at * batch, batch), :] = a
    low = jnp.dot(both_ref[pl.ds(pair, pair), :], down_ref[...], preferred_element_type=F32)
    dlow = lax.dot_general(
        both_ref[pl.ds(0, pair), :],
        up_ref[...],
        (((1,), (1,)), ((), ())),
        preferred_element_type=F32,
    )
    none = jnp.zeros((pair, part), F32)
    columns = []
    for ry in range(tall):
        owner = 2 * lax.rem(y + ry, tall) + core
        lo, dl = none, none
        for t in range(owners):
            lo = jnp.where(owner == t, low[:, t * part : (t + 1) * part], lo)
            dl = jnp.where(owner == t, dlow[:, t * part : (t + 1) * part], dl)
        columns.append(
            jnp.concatenate(
                [jnp.concatenate([lo, none], axis=1), jnp.concatenate([none, dl], axis=1)], axis=0
            )
        )
    right = jnp.concatenate(columns, axis=1).astype(BF16)
    step = math.gcd(wide, 384)
    for d in range(0, wide, step):
        sum_ref[pl.ds(d, step), :] = lax.dot_general(
            both_ref[:, d : d + step], right, (((0,), (0,)), ((), ())), preferred_element_type=F32
        )
    each = wide // groups
    block = 2 * part
    for r in range(far):
        for rx in range(2):
            g = 2 * lax.rem(z + r, far) + (x + rx - 2 * x * rx)
            start = pl.multiple_of(g * each, 16)
            for ry in range(tall):
                out = outs[rx * tall + ry]
                cols = slice(ry * block, (ry + 1) * block)
                out[r] = sum_ref[pl.ds(start, each), cols].astype(out.dtype)


def part_grads(pos, x, ct, xs, cts, down, up, owners, groups):
    wide, rank = down.shape
    batch = x.shape[0]
    tall, far = owners // 2, groups // 2
    block = 2 * (rank // owners)
    shape = (far, wide // groups, block)
    return pl.pallas_call(
        functools.partial(grads_kernel, owners=owners, groups=groups),
        in_specs=[whole(pltpu.SMEM)] + [whole()] * 6,
        out_specs=[whole()] * (2 * tall),
        out_shape=[jax.ShapeDtypeStruct(shape, BF16 if i else F32) for i in range(2 * tall)],
        scratch_shapes=[
            pltpu.VMEM((4 * batch, wide), BF16),
            pltpu.VMEM((wide, tall * block), F32),
        ],
        compiler_params=room(24),
        name="part_grads",
    )(pos, in_hbm(x), in_hbm(ct), xs, cts, in_hbm(down), in_hbm(up))


def fold_kernel(keep, *refs, far):
    came, outs = refs[:-far], refs[-far:]
    for r in range(far):
        total = keep[r]
        for one in came:
            total = total + one[r].astype(F32)
        outs[r][...] = total.astype(outs[r].dtype)


def fold(keep, came):
    far, rows, block = keep.shape
    return pl.pallas_call(
        functools.partial(fold_kernel, far=far),
        in_specs=[whole()] * (1 + len(came)),
        out_specs=[whole()] * far,
        out_shape=[jax.ShapeDtypeStruct((rows, block), BF16 if r else F32) for r in range(far)],
        compiler_params=room(12),
        name="fold",
    )(keep, *came)


def finish_kernel(*refs, factor):
    up_ref, down_ref = refs[-2:]
    total = refs[0][...]
    for r in refs[1:-2]:
        total = total + r[...].astype(F32)
    total = total * factor
    half = total.shape[1] // 2
    flat = total.T
    up_ref[...] = flat[:half, :]
    down_ref[...] = flat[half:, :]


def finish(keep, came, factor):
    rows, block = keep.shape
    half = block // 2
    shape = jax.ShapeDtypeStruct
    up, down = pl.pallas_call(
        functools.partial(finish_kernel, factor=factor),
        in_specs=[whole()] * (1 + len(came)),
        out_specs=[whole()] * 2,
        out_shape=[shape((half, rows), F32)] * 2,
        compiler_params=room(8),
        name="finish",
    )(keep, *came)
    return up, down.T


def exchange_start(x, ct, up, down, after):
    owners, groups = lax.axis_size("tbl"), lax.axis_size("grp")
    tall = owners // 2
    t, g = lax.axis_index("tbl"), lax.axis_index("grp")
    pos = jnp.stack([t % 2, t // 2, g % 2, g // 2]).astype(jnp.int32)
    other_core = [(i, i ^ 1) for i in range(owners)]
    xs = lax.ppermute(x, "tbl", other_core)
    cts = lax.ppermute(ct, "tbl", other_core)
    xs, cts, after = lax.optimization_barrier((xs, cts, after))
    parts = part_grads(pos, x, ct, xs, cts, down, up, owners, groups)

    def to(rx, ry):
        return [
            (i * owners + j, (i ^ rx) * owners + 2 * ((j // 2 + ry) % tall) + j % 2)
            for i in range(groups)
            for j in range(owners)
        ]

    came = []
    for i in range(1, 2 * tall):
        came.append(lax.ppermute(parts[i], ("grp", "tbl"), to(i // tall, i % tall)))
    return parts[0], came, after


def exchange_end(keep, came, factor):
    groups = lax.axis_size("grp")
    far = groups // 2

    def to_z(r):
        return [(i, 2 * ((i // 2 + r) % far) + i % 2) for i in range(groups)]

    out = fold(keep, came)
    last = []
    for r in range(1, far):
        last.append(lax.ppermute(out[r], "grp", to_z(r)))
    return finish(out[0], last, factor)


def grads_plain(x, ct, up, down, factor):
    low = jnp.dot(x, down, preferred_element_type=F32).astype(BF16)
    dz = (ct.astype(F32) * x.astype(F32)).astype(BF16)
    dlow = jnp.dot(dz, up.T, preferred_element_type=F32).astype(BF16)
    part_up = jnp.dot(low.T, dz, preferred_element_type=F32) * factor
    part_down = jnp.dot(x.T, dlow, preferred_element_type=F32) * factor
    owner_up = lax.psum_scatter(part_up, "tbl", scatter_dimension=0, tiled=True)
    owner_down = lax.psum_scatter(part_down, "tbl", scatter_dimension=1, tiled=True)
    return (
        lax.psum_scatter(owner_up, "grp", scatter_dimension=1, tiled=True),
        lax.psum_scatter(owner_down, "grp", scatter_dimension=0, tiled=True),
    )


def on_device(ids, lengths, slot_of_table, tables, x, ct, up, down):
    owners, groups = lax.axis_size("tbl"), lax.axis_size("grp")
    batch = ids.shape[0]
    slots, rows = tables.shape[:2]
    maxlen = ids.shape[1] // (slots * owners)
    factor = 1.0 / math.sqrt(batch * owners * groups)
    tiled = by_exchange(owners, groups, *down.shape)

    masked = mask_ids(slot_of_table, ids, lengths, maxlen, rows)
    if tiled:
        keep, came, masked = exchange_start(x, ct, up, down, masked)
    got = lax.all_to_all(masked.reshape(owners, slots * maxlen, batch), "tbl", 0, 0)
    if tiled:
        got, keep = lax.optimization_barrier((got, keep))
    firsts, counts = (0,), (slots,)
    parts = []
    for first, count in zip(firsts, counts):
        pooled = pool_slots(got, tables, first, count, maxlen)
        parts.append(lax.all_to_all(pooled, "tbl", 0, 0))
    embedded = place(slot_of_table, parts, firsts, counts, slots)
    if tiled:
        grad_up, grad_down = exchange_end(keep, came, factor)
    else:
        grad_up, grad_down = grads_plain(x, ct, up, down, factor)
    return embedded, grad_up, grad_down


def by_exchange(owners, groups, wide, rank):
    each, part = wide // groups, rank // owners
    return owners % 2 == 0 and groups % 2 == 0 and each % 16 == 0 and 2 * part % LANES == 0


def solution(mesh):
    rows = P(("grp", "tbl"), None)
    return jax.shard_map(
        on_device,
        mesh=mesh,
        in_specs=(rows, rows, P(), P("tbl", None, None), rows, rows, P(), P()),
        out_specs=(rows, P("tbl", "grp"), P("grp", "tbl")),
        check_vma=False,
    )
```

```python
import functools
import math

import jax
import jax.numpy as jnp
from jax import lax
from jax.experimental import pallas as pl
from jax.experimental.pallas import tpu as pltpu
from jax.sharding import PartitionSpec as P


F32 = jnp.float32
BF16 = jnp.bfloat16
LANES = 128


def room(mebibytes):
    return pltpu.CompilerParams(vmem_limit_bytes=mebibytes * 2**20)


def whole(memory=pltpu.VMEM):
    return pl.BlockSpec(memory_space=memory)


def in_hbm(x):
    return pltpu.with_memory_space_constraint(x, pltpu.HBM)


def mask_ids_kernel(slot_ref, ids_ref, lens_ref, out_ref, *, maxlen, rows):
    entries, batch = out_ref.shape
    feats = lens_ref.shape[0]
    slot_of_row = lax.broadcasted_iota(jnp.int32, (entries, feats), 0) // maxlen
    hit = (slot_of_row == slot_ref[...]).astype(F32)
    lens = jnp.dot(hit, lens_ref[...].astype(F32), preferred_element_type=F32)
    place = lax.broadcasted_iota(jnp.int32, (entries, batch), 0) % maxlen
    keep = place.astype(F32) + 0.5 < lens
    out_ref[...] = jnp.where(keep, ids_ref[...], rows)


def mask_ids(slot_of_table, ids, lengths, maxlen, rows):
    return pl.pallas_call(
        functools.partial(mask_ids_kernel, maxlen=maxlen, rows=rows),
        in_specs=[whole()] * 3,
        out_specs=whole(),
        out_shape=jax.ShapeDtypeStruct((ids.shape[1], ids.shape[0]), jnp.int32),
        compiler_params=room(4),
        name="mask_ids",
    )(in_hbm(slot_of_table.reshape(1, -1)), in_hbm(ids.T), in_hbm(lengths.T))


def pool_kernel(ids_ref, table_ref, out_ref, wide_ref, sum_ref, *rest, first, chunk):
    rows, width = table_ref.shape[1:]
    groups, _, batch, _ = out_ref.shape
    near, sem = rest[:groups], rest[groups]
    maxlen = near[0].shape[0]
    step, steps = pl.program_id(0), pl.num_programs(0)

    def fetch(g, at):
        start = pl.multiple_of((first + at) * maxlen, maxlen)
        return pltpu.make_async_copy(ids_ref.at[g, pl.ds(start, maxlen)], near[g], sem.at[g])

    @pl.when(step == 0)
    def _():
        for g in range(groups):
            fetch(g, 0).start()

    def widen(i, carry):
        start = pl.multiple_of(i * chunk, chunk)
        wide_ref[pl.ds(start, chunk), :] = table_ref[0, pl.ds(start, chunk), :].astype(F32)
        return carry

    lax.fori_loop(0, rows // chunk, widen, 0)
    wide_ref[pl.ds(rows, 8), :] = jnp.zeros((8, width), F32)
    for g in range(groups):
        fetch(g, step).wait()
        for b in range(batch):
            total = wide_ref[pl.ds(near[g][0, b], 1), :]
            for k in range(1, maxlen):
                total = total + wide_ref[pl.ds(near[g][k, b], 1), :]
            sum_ref[pl.ds(b, 1), :] = total
        out_ref[g, 0] = sum_ref[...].astype(BF16)

        @pl.when(step + 1 < steps)
        def _(g=g):
            fetch(g, step + 1).start()


def pool_slots(ids, tables, first, count, maxlen):
    groups, _, batch = ids.shape
    rows, width = tables.shape[1:]
    return pl.pallas_call(
        functools.partial(pool_kernel, first=first, chunk=math.gcd(rows, 512)),
        grid=(count,),
        in_specs=[
            pl.BlockSpec(memory_space=pl.ANY),
            pl.BlockSpec((1, rows, width), lambda s: (s + first, 0, 0)),
        ],
        out_specs=pl.BlockSpec((groups, 1, batch, width), lambda s: (0, s, 0, 0)),
        out_shape=jax.ShapeDtypeStruct((groups, count, batch, width), BF16),
        scratch_shapes=[pltpu.VMEM((rows + 8, width), F32), pltpu.VMEM((batch, width), F32)]
        + [pltpu.SMEM((maxlen, batch), jnp.int32)] * groups
        + [pltpu.SemaphoreType.DMA((groups,))],
        compiler_params=room(12),
        name="pool_slots",
    )(ids, in_hbm(tables))


def place_kernel(slot_ref, *refs, slots, firsts, counts):
    parts, out_ref, sem = refs[:-2], refs[-2], refs[-1]
    width = parts[0].shape[3]
    feats = slot_ref.shape[0]

    def put(f, part, owner, local):
        to = out_ref.at[:, pl.ds(f * width, width)]
        return pltpu.make_async_copy(part.at[owner, local], to, sem.at[f])

    for f in range(feats):
        slot = slot_ref[f]
        owner = slot // slots
        local = slot - owner * slots
        for part, first, count in zip(parts, firsts, counts):
            if len(parts) == 1:
                put(f, part, owner, local).start()
            else:

                @pl.when((local >= first) & (local < first + count))
                def _(f=f, part=part, owner=owner, at=local - first):
                    put(f, part, owner, at).start()

    for f in range(feats):
        put(f, parts[0], 0, 0).wait()


def place(slot_of_table, parts, firsts, counts, slots):
    batch, width = parts[0].shape[2:]
    feats = slot_of_table.shape[0]
    return pl.pallas_call(
        functools.partial(place_kernel, slots=slots, firsts=firsts, counts=counts),
        in_specs=[whole(pltpu.SMEM)] + [whole(pl.ANY)] * len(parts),
        out_specs=whole(pl.ANY),
        out_shape=jax.ShapeDtypeStruct((batch, feats * width), BF16),
        scratch_shapes=[pltpu.SemaphoreType.DMA((feats,))],
        compiler_params=room(4),
        name="place",
    )(slot_of_table, *parts)


def grads_kernel(pos_ref, xs_ref, cts_ref, x_hbm, ct_hbm, down_hbm, up_hbm, *refs, owners, groups):
    tall, far = owners // 2, groups // 2
    outs = refs[: 2 * tall]
    both_ref, sum_ref, x_ref, ct_ref, down_ref, up_ref, sem = refs[2 * tall :]
    core, y, x, z = pos_ref[0] & 1, pos_ref[0] >> 1, pos_ref[1] & 1, pos_ref[1] >> 1
    batch, wide = x_ref.shape
    rank = down_ref.shape[1]
    part = rank // owners
    pair = 2 * batch
    loads = [
        pltpu.make_async_copy(src, dst, sem.at[i])
        for i, (src, dst) in enumerate(
            ((x_hbm, x_ref), (ct_hbm, ct_ref), (down_hbm, down_ref), (up_hbm, up_ref))
        )
    ]
    for load in loads:
        load.start()
    for at, (a_ref, b_ref) in enumerate(((xs_ref, cts_ref), (x_ref, ct_ref))):
        if at:
            loads[0].wait()
            loads[1].wait()
        a = a_ref[...]
        both_ref[pl.ds(at * batch, batch), :] = (b_ref[...].astype(F32) * a.astype(F32)).astype(BF16)
        both_ref[pl.ds(pair + at * batch, batch), :] = a
    loads[2].wait()
    low = jnp.dot(both_ref[pl.ds(pair, pair), :], down_ref[...], preferred_element_type=F32)
    loads[3].wait()
    dlow = lax.dot_general(
        both_ref[pl.ds(0, pair), :],
        up_ref[...],
        (((1,), (1,)), ((), ())),
        preferred_element_type=F32,
    )
    none = jnp.zeros((pair, part), F32)
    columns = []
    for ry in range(tall):
        owner = 2 * lax.rem(y + ry, tall) + core
        lo, dl = none, none
        for t in range(owners):
            lo = jnp.where(owner == t, low[:, t * part : (t + 1) * part], lo)
            dl = jnp.where(owner == t, dlow[:, t * part : (t + 1) * part], dl)
        columns.append(
            jnp.concatenate(
                [jnp.concatenate([lo, none], axis=1), jnp.concatenate([none, dl], axis=1)], axis=0
            )
        )
    right = jnp.concatenate(columns, axis=1).astype(BF16)
    step = math.gcd(wide, 384)
    for d in range(0, wide, step):
        sum_ref[pl.ds(d, step), :] = lax.dot_general(
            both_ref[:, d : d + step], right, (((0,), (0,)), ((), ())), preferred_element_type=F32
        )
    each = wide // groups
    block = 2 * part
    for r in range(far):
        for rx in range(2):
            g = 2 * lax.rem(z + r, far) + (x + rx - 2 * x * rx)
            start = pl.multiple_of(g * each, 16)
            for ry in range(tall):
                out = outs[rx * tall + ry]
                cols = slice(ry * block, (ry + 1) * block)
                out[r] = sum_ref[pl.ds(start, each), cols].astype(out.dtype)


def part_grads(pos, x, ct, xs, cts, down, up, owners, groups):
    wide, rank = down.shape
    batch = x.shape[0]
    tall, far = owners // 2, groups // 2
    block = 2 * (rank // owners)
    shape = (far, wide // groups, block)
    return pl.pallas_call(
        functools.partial(grads_kernel, owners=owners, groups=groups),
        in_specs=[whole(pltpu.SMEM)] + [whole()] * 2 + [whole(pl.ANY)] * 4,
        out_specs=[whole()] * (2 * tall),
        out_shape=[pltpu.VMEM(shape, BF16 if i else F32) for i in range(2 * tall)],
        scratch_shapes=[
            pltpu.VMEM((4 * batch, wide), BF16),
            pltpu.VMEM((wide, tall * block), F32),
        ]
        + [pltpu.VMEM(a.shape, BF16) for a in (x, ct, down, up)]
        + [pltpu.SemaphoreType.DMA((4,))],
        compiler_params=room(24),
        name="part_grads",
    )(pos, xs, cts, in_hbm(x), in_hbm(ct), in_hbm(down), in_hbm(up))


def fold_kernel(keep, *refs, far):
    came, outs = refs[:-far], refs[-far:]
    for r in range(far):
        total = keep[r]
        for one in came:
            total = total + one[r].astype(F32)
        outs[r][...] = total.astype(outs[r].dtype)


def fold(keep, came):
    far, rows, block = keep.shape
    return pl.pallas_call(
        functools.partial(fold_kernel, far=far),
        in_specs=[whole()] * (1 + len(came)),
        out_specs=[whole()] * far,
        out_shape=[jax.ShapeDtypeStruct((rows, block), BF16 if r else F32) for r in range(far)],
        compiler_params=room(12),
        name="fold",
    )(keep, *came)


def finish_kernel(*refs, factor):
    up_ref, down_ref = refs[-2:]
    total = refs[0][...]
    for r in refs[1:-2]:
        total = total + r[...].astype(F32)
    total = total * factor
    half = total.shape[1] // 2
    flat = total.T
    up_ref[...] = flat[:half, :]
    down_ref[...] = flat[half:, :]


def finish(keep, came, factor):
    rows, block = keep.shape
    half = block // 2
    shape = jax.ShapeDtypeStruct
    up, down = pl.pallas_call(
        functools.partial(finish_kernel, factor=factor),
        in_specs=[whole()] * (1 + len(came)),
        out_specs=[whole()] * 2,
        out_shape=[shape((half, rows), F32)] * 2,
        compiler_params=room(8),
        name="finish",
    )(keep, *came)
    return up, down.T


def exchange_start(x, ct, up, down, after):
    owners, groups = lax.axis_size("tbl"), lax.axis_size("grp")
    tall = owners // 2
    t, g = lax.axis_index("tbl"), lax.axis_index("grp")
    pos = jnp.stack([t, g]).astype(jnp.int32)
    other_core = [(i, i ^ 1) for i in range(owners)]
    xs = lax.ppermute(x, "tbl", other_core)
    cts = lax.ppermute(ct, "tbl", other_core)
    xs, cts, after = lax.optimization_barrier((xs, cts, after))
    parts = part_grads(pos, x, ct, xs, cts, down, up, owners, groups)

    def to(rx, ry):
        return [
            (i * owners + j, (i ^ rx) * owners + 2 * ((j // 2 + ry) % tall) + j % 2)
            for i in range(groups)
            for j in range(owners)
        ]

    came = []
    for i in range(1, 2 * tall):
        came.append(lax.ppermute(parts[i], ("grp", "tbl"), to(i // tall, i % tall)))
    return parts[0], came, after


def exchange_end(keep, came, factor):
    groups = lax.axis_size("grp")
    far = groups // 2

    def to_z(r):
        return [(i, 2 * ((i // 2 + r) % far) + i % 2) for i in range(groups)]

    out = fold(keep, came)
    last = []
    for r in range(1, far):
        last.append(lax.ppermute(out[r], "grp", to_z(r)))
    return finish(out[0], last, factor)


def grads_plain(x, ct, up, down, factor):
    low = jnp.dot(x, down, preferred_element_type=F32).astype(BF16)
    dz = (ct.astype(F32) * x.astype(F32)).astype(BF16)
    dlow = jnp.dot(dz, up.T, preferred_element_type=F32).astype(BF16)
    part_up = jnp.dot(low.T, dz, preferred_element_type=F32) * factor
    part_down = jnp.dot(x.T, dlow, preferred_element_type=F32) * factor
    owner_up = lax.psum_scatter(part_up, "tbl", scatter_dimension=0, tiled=True)
    owner_down = lax.psum_scatter(part_down, "tbl", scatter_dimension=1, tiled=True)
    return (
        lax.psum_scatter(owner_up, "grp", scatter_dimension=1, tiled=True),
        lax.psum_scatter(owner_down, "grp", scatter_dimension=0, tiled=True),
    )


def on_device(ids, lengths, slot_of_table, tables, x, ct, up, down):
    owners, groups = lax.axis_size("tbl"), lax.axis_size("grp")
    batch = ids.shape[0]
    slots, rows = tables.shape[:2]
    maxlen = ids.shape[1] // (slots * owners)
    factor = 1.0 / math.sqrt(batch * owners * groups)
    tiled = by_exchange(owners, groups, *down.shape)

    masked = mask_ids(slot_of_table, ids, lengths, maxlen, rows)
    if tiled:
        keep, came, masked = exchange_start(x, ct, up, down, masked)
    got = lax.all_to_all(masked.reshape(owners, slots * maxlen, batch), "tbl", 0, 0)
    if tiled:
        got, keep = lax.optimization_barrier((got, keep))
    firsts, counts = (0,), (slots,)
    parts = []
    for first, count in zip(firsts, counts):
        pooled = pool_slots(got, tables, first, count, maxlen)
        parts.append(lax.all_to_all(pooled, "tbl", 0, 0))
    embedded = place(slot_of_table, parts, firsts, counts, slots)
    if tiled:
        grad_up, grad_down = exchange_end(keep, came, factor)
    else:
        grad_up, grad_down = grads_plain(x, ct, up, down, factor)
    return embedded, grad_up, grad_down


def by_exchange(owners, groups, wide, rank):
    each, part = wide // groups, rank // owners
    return owners % 2 == 0 and groups % 2 == 0 and each % 16 == 0 and 2 * part % LANES == 0


def solution(mesh):
    rows = P(("grp", "tbl"), None)
    return jax.shard_map(
        on_device,
        mesh=mesh,
        in_specs=(rows, rows, P(), P("tbl", None, None), rows, rows, P(), P()),
        out_specs=(rows, P("tbl", "grp"), P("grp", "tbl")),
        check_vma=False,
    )
```

```python
import functools
import math

import jax
import jax.numpy as jnp
from jax import lax
from jax.experimental import pallas as pl
from jax.experimental.pallas import tpu as pltpu
from jax.sharding import PartitionSpec as P


F32 = jnp.float32
BF16 = jnp.bfloat16
LANES = 128


def room(mebibytes):
    return pltpu.CompilerParams(vmem_limit_bytes=mebibytes * 2**20)


def whole(memory=pltpu.VMEM):
    return pl.BlockSpec(memory_space=memory)


def in_hbm(x):
    return pltpu.with_memory_space_constraint(x, pltpu.HBM)


def masked_ids(slot_ref, ids_ref, lens_ref, maxlen, rows):
    entries, batch = ids_ref.shape
    feats = lens_ref.shape[0]
    slot_of_row = lax.broadcasted_iota(jnp.int32, (entries, feats), 0) // maxlen
    hit = (slot_of_row == slot_ref[...]).astype(F32)
    lens = jnp.dot(hit, lens_ref[...].astype(F32), preferred_element_type=F32)
    place = lax.broadcasted_iota(jnp.int32, (entries, batch), 0) % maxlen
    keep = place.astype(F32) + 0.5 < lens
    return jnp.where(keep, ids_ref[...], rows)


def mask_kernel(slot_ref, ids_ref, lens_ref, out_ref, *, maxlen, rows):
    out_ref[...] = masked_ids(slot_ref, ids_ref, lens_ref, maxlen, rows)


def mask_ids(slot_of_table, ids, lengths, maxlen, rows):
    return pl.pallas_call(
        functools.partial(mask_kernel, maxlen=maxlen, rows=rows),
        in_specs=[whole()] * 3,
        out_specs=whole(),
        out_shape=jax.ShapeDtypeStruct((ids.shape[1], ids.shape[0]), jnp.int32),
        compiler_params=room(4),
        name="mask_ids",
    )(slot_of_table.reshape(1, -1), ids.T, lengths.T)


def prep_kernel(*refs, maxlen, rows):
    sources, (masked_ref, rank_ref), targets, sem = refs[:7], refs[7:9], refs[9:16], refs[16]
    slot_ref, ids_ref, lens_ref, x_ref, ct_ref, down_ref, up_ref = targets
    loads = [
        pltpu.make_async_copy(src, dst, sem.at[i]) for i, (src, dst) in enumerate(zip(sources, targets))
    ]
    for load in loads:
        load.start()
    for load in loads[:3]:
        load.wait()
    masked_ref[...] = masked_ids(slot_ref, ids_ref, lens_ref, maxlen, rows)
    for load in loads[3:5]:
        load.wait()
    x = x_ref[...]
    dz = (ct_ref[...].astype(F32) * x.astype(F32)).astype(BF16)
    loads[5].wait()
    rank_ref[0] = jnp.dot(x, down_ref[...], preferred_element_type=F32).astype(BF16)
    loads[6].wait()
    rank_ref[1] = lax.dot_general(
        dz, up_ref[...], (((1,), (1,)), ((), ())), preferred_element_type=F32
    ).astype(BF16)


def prep(slot_of_table, ids, lengths, x, ct, down, up, maxlen, rows):
    sources = [slot_of_table.reshape(1, -1), ids.T, lengths.T, x, ct, down, up]
    return pl.pallas_call(
        functools.partial(prep_kernel, maxlen=maxlen, rows=rows),
        in_specs=[whole(pl.ANY)] * 7,
        out_specs=[whole()] * 2,
        out_shape=[
            jax.ShapeDtypeStruct(ids.shape[::-1], jnp.int32),
            jax.ShapeDtypeStruct((2, x.shape[0], down.shape[1]), BF16),
        ],
        scratch_shapes=[pltpu.VMEM(a.shape, a.dtype) for a in sources]
        + [pltpu.SemaphoreType.DMA((7,))],
        compiler_params=room(16),
        name="prep",
    )(*[in_hbm(a) for a in sources])


def pool_kernel(ids_ref, table_ref, out_ref, wide_ref, sum_ref, *rest, first, chunk):
    rows, width = table_ref.shape[1:]
    groups, _, batch, _ = out_ref.shape
    near, sem = rest[:groups], rest[groups]
    maxlen = near[0].shape[0]
    step, steps = pl.program_id(0), pl.num_programs(0)

    def fetch(g, at):
        start = pl.multiple_of((first + at) * maxlen, maxlen)
        return pltpu.make_async_copy(ids_ref.at[g, pl.ds(start, maxlen)], near[g], sem.at[g])

    @pl.when(step == 0)
    def _():
        for g in range(groups):
            fetch(g, 0).start()

    def widen(i, carry):
        start = pl.multiple_of(i * chunk, chunk)
        wide_ref[pl.ds(start, chunk), :] = table_ref[0, pl.ds(start, chunk), :].astype(F32)
        return carry

    lax.fori_loop(0, rows // chunk, widen, 0)
    wide_ref[pl.ds(rows, 8), :] = jnp.zeros((8, width), F32)
    for g in range(groups):
        fetch(g, step).wait()
        for b in range(batch):
            total = wide_ref[pl.ds(near[g][0, b], 1), :]
            for k in range(1, maxlen):
                total = total + wide_ref[pl.ds(near[g][k, b], 1), :]
            sum_ref[pl.ds(b, 1), :] = total
        out_ref[g, 0] = sum_ref[...].astype(BF16)

        @pl.when(step + 1 < steps)
        def _(g=g):
            fetch(g, step + 1).start()


def pool_slots(ids, tables, first, count, maxlen):
    groups, _, batch = ids.shape
    rows, width = tables.shape[1:]
    return pl.pallas_call(
        functools.partial(pool_kernel, first=first, chunk=math.gcd(rows, 512)),
        grid=(count,),
        in_specs=[
            pl.BlockSpec(memory_space=pl.ANY),
            pl.BlockSpec((1, rows, width), lambda s: (s + first, 0, 0)),
        ],
        out_specs=pl.BlockSpec((groups, 1, batch, width), lambda s: (0, s, 0, 0)),
        out_shape=jax.ShapeDtypeStruct((groups, count, batch, width), BF16),
        scratch_shapes=[pltpu.VMEM((rows + 8, width), F32), pltpu.VMEM((batch, width), F32)]
        + [pltpu.SMEM((maxlen, batch), jnp.int32)] * groups
        + [pltpu.SemaphoreType.DMA((groups,))],
        compiler_params=room(12),
        name="pool_slots",
    )(ids, in_hbm(tables))


def place_kernel(slot_ref, *refs, slots, firsts, counts):
    parts, out_ref, sem = refs[:-2], refs[-2], refs[-1]
    width = parts[0].shape[3]
    feats = slot_ref.shape[0]

    def put(f, part, owner, local):
        to = out_ref.at[:, pl.ds(f * width, width)]
        return pltpu.make_async_copy(part.at[owner, local], to, sem.at[f])

    for f in range(feats):
        slot = slot_ref[f]
        owner = slot // slots
        local = slot - owner * slots
        for part, first, count in zip(parts, firsts, counts):
            if len(parts) == 1:
                put(f, part, owner, local).start()
            else:

                @pl.when((local >= first) & (local < first + count))
                def _(f=f, part=part, owner=owner, at=local - first):
                    put(f, part, owner, at).start()

    for f in range(feats):
        put(f, parts[0], 0, 0).wait()


def place(slot_of_table, parts, firsts, counts, slots):
    batch, width = parts[0].shape[2:]
    feats = slot_of_table.shape[0]
    return pl.pallas_call(
        functools.partial(place_kernel, slots=slots, firsts=firsts, counts=counts),
        in_specs=[whole(pltpu.SMEM)] + [whole(pl.ANY)] * len(parts),
        out_specs=whole(pl.ANY),
        out_shape=jax.ShapeDtypeStruct((batch, feats * width), BF16),
        scratch_shapes=[pltpu.SemaphoreType.DMA((feats,))],
        compiler_params=room(4),
        name="place",
    )(slot_of_table, *parts)


def grads_kernel(pos_ref, own_ref, sib_ref, *refs, owners, groups, chunks):
    tall, far = owners // 2, groups // 2
    sources, keep_ref, sends = refs[:4], refs[4], refs[5 : 4 + 2 * tall]
    both_ref, sum_ref, near_ref, in_sem, sem = refs[4 + 2 * tall : 9 + 2 * tall]
    targets = refs[9 + 2 * tall :]
    g, t = lax.div(pos_ref[0], owners), lax.rem(pos_ref[0], owners)
    core, y, x, z = t & 1, t >> 1, g & 1, g >> 1
    batch, wide = sources[0].shape
    part = own_ref.shape[2] // owners
    pair = 2 * batch
    span = wide // chunks
    loads = []
    for c in range(chunks):
        at = pl.ds(c * span, span)
        loads.append(
            [
                pltpu.make_async_copy(src.at[:, at], dst.at[:, at], in_sem.at[4 * c + i])
                for i, (src, dst) in enumerate(zip(sources, targets))
            ]
        )
        for load in loads[-1]:
            load.start()
    low = jnp.concatenate([own_ref[0], sib_ref[0]], axis=0).astype(F32)
    dlow = jnp.concatenate([own_ref[1], sib_ref[1]], axis=0).astype(F32)
    none = jnp.zeros((pair, part), F32)
    columns = []
    for ry in range(tall):
        owner = 2 * lax.rem(y + ry, tall) + core
        lo, dl = none, none
        for t in range(owners):
            lo = jnp.where(owner == t, low[:, t * part : (t + 1) * part], lo)
            dl = jnp.where(owner == t, dlow[:, t * part : (t + 1) * part], dl)
        columns.append(
            jnp.concatenate(
                [jnp.concatenate([lo, none], axis=1), jnp.concatenate([none, dl], axis=1)], axis=0
            )
        )
    right = jnp.concatenate(columns, axis=1).astype(BF16)
    step = math.gcd(span, 384)
    for c in range(chunks):
        for load in loads[c]:
            load.wait()
        for d in range(c * span, (c + 1) * span, step):
            cols = slice(d, d + step)
            for i in range(2):
                a = targets[2 * i][:, cols]
                dz = targets[2 * i + 1][:, cols].astype(F32) * a.astype(F32)
                both_ref[pl.ds(i * batch, batch), :] = dz.astype(BF16)
                both_ref[pl.ds(pair + i * batch, batch), :] = a
            sum_ref[pl.ds(d, step), :] = lax.dot_general(
                both_ref[...], right, (((0,), (0,)), ((), ())), preferred_element_type=F32
            )
    each = wide // groups
    block = 2 * part
    copies = []
    for i in range(2 * tall - 1, -1, -1):
        rx, ry = i // tall, i % tall
        cols = slice(ry * block, (ry + 1) * block)
        for r in range(far):
            g = 2 * lax.rem(z + r, far) + (x + rx - 2 * x * rx)
            found = sum_ref[pl.ds(pl.multiple_of(g * each, 16), each), cols]
            if i:
                near_ref[i - 1, r] = found.astype(BF16)
            else:
                keep_ref[r] = found
        if i:
            copies.append(pltpu.make_async_copy(near_ref.at[i - 1], sends[i - 1], sem.at[i - 1]))
            copies[-1].start()
    for copy in copies:
        copy.wait()


def part_grads(pos, own, sib, x, ct, xs, cts, owners, groups):
    batch, wide = x.shape
    rank = own.shape[2]
    tall, far = owners // 2, groups // 2
    block = 2 * (rank // owners)
    shape = (far, wide // groups, block)
    others = 2 * tall - 1
    chunks = 3 if wide % (3 * LANES) == 0 else 1
    step = math.gcd(wide // chunks, 384)
    return pl.pallas_call(
        functools.partial(grads_kernel, owners=owners, groups=groups, chunks=chunks),
        in_specs=[whole(pltpu.SMEM)] + [whole()] * 2 + [whole(pl.ANY)] * 4,
        out_specs=[whole()] + [whole(pl.ANY)] * others,
        out_shape=[jax.ShapeDtypeStruct(shape, F32)] + [jax.ShapeDtypeStruct(shape, BF16)] * others,
        scratch_shapes=[
            pltpu.VMEM((4 * batch, step), BF16),
            pltpu.VMEM((wide, tall * block), F32),
            pltpu.VMEM((others, *shape), BF16),
            pltpu.SemaphoreType.DMA((4 * chunks,)),
            pltpu.SemaphoreType.DMA((others,)),
        ]
        + [pltpu.VMEM((batch, wide), BF16)] * 4,
        compiler_params=room(20),
        name="part_grads",
    )(pos, own, sib, in_hbm(x), in_hbm(ct), xs, cts)


def fold_kernel(keep, *refs, far):
    came, outs = refs[:-far], refs[-far:]
    for r in range(far):
        total = keep[r]
        for one in came:
            total = total + one[r].astype(F32)
        outs[r][...] = total.astype(outs[r].dtype)


def fold(keep, came):
    far, rows, block = keep.shape
    return pl.pallas_call(
        functools.partial(fold_kernel, far=far),
        in_specs=[whole()] * (1 + len(came)),
        out_specs=[whole()] * far,
        out_shape=[jax.ShapeDtypeStruct((rows, block), BF16 if r else F32) for r in range(far)],
        compiler_params=room(12),
        name="fold",
    )(keep, *came)


def finish_kernel(*refs, factor):
    up_ref, down_ref = refs[-2:]
    total = refs[0][...]
    for r in refs[1:-2]:
        total = total + r[...].astype(F32)
    total = total * factor
    half = total.shape[1] // 2
    flat = total.T
    up_ref[...] = flat[:half, :]
    down_ref[...] = flat[half:, :]


def finish(keep, came, factor):
    rows, block = keep.shape
    half = block // 2
    shape = jax.ShapeDtypeStruct
    up, down = pl.pallas_call(
        functools.partial(finish_kernel, factor=factor),
        in_specs=[whole()] * (1 + len(came)),
        out_specs=[whole()] * 2,
        out_shape=[shape((half, rows), F32)] * 2,
        compiler_params=room(8),
        name="finish",
    )(keep, *came)
    return up, down.T


def exchange_start(x, ct, own):
    owners, groups = lax.axis_size("tbl"), lax.axis_size("grp")
    tall = owners // 2
    pos = lax.axis_index(("grp", "tbl")).astype(jnp.int32).reshape(1)
    other_core = [(i, i ^ 1) for i in range(owners)]
    xs = lax.ppermute(x, "tbl", other_core)
    cts = lax.ppermute(ct, "tbl", other_core)
    sib = lax.ppermute(own, "tbl", other_core)
    parts = part_grads(pos, own, sib, x, ct, xs, cts, owners, groups)

    def to(rx, ry):
        return [
            (i * owners + j, (i ^ rx) * owners + 2 * ((j // 2 + ry) % tall) + j % 2)
            for i in range(groups)
            for j in range(owners)
        ]

    came = []
    for i in range(1, 2 * tall):
        came.append(lax.ppermute(parts[i], ("grp", "tbl"), to(i // tall, i % tall)))
    return parts[0], came


def exchange_end(keep, came, factor):
    groups = lax.axis_size("grp")
    far = groups // 2

    def to_z(r):
        return [(i, 2 * ((i // 2 + r) % far) + i % 2) for i in range(groups)]

    out = fold(keep, came)
    last = []
    for r in range(1, far):
        last.append(lax.ppermute(out[r], "grp", to_z(r)))
    return finish(out[0], last, factor)


def grads_plain(x, ct, up, down, factor):
    low = jnp.dot(x, down, preferred_element_type=F32).astype(BF16)
    dz = (ct.astype(F32) * x.astype(F32)).astype(BF16)
    dlow = jnp.dot(dz, up.T, preferred_element_type=F32).astype(BF16)
    part_up = jnp.dot(low.T, dz, preferred_element_type=F32) * factor
    part_down = jnp.dot(x.T, dlow, preferred_element_type=F32) * factor
    owner_up = lax.psum_scatter(part_up, "tbl", scatter_dimension=0, tiled=True)
    owner_down = lax.psum_scatter(part_down, "tbl", scatter_dimension=1, tiled=True)
    return (
        lax.psum_scatter(owner_up, "grp", scatter_dimension=1, tiled=True),
        lax.psum_scatter(owner_down, "grp", scatter_dimension=0, tiled=True),
    )


def on_device(ids, lengths, slot_of_table, tables, x, ct, up, down):
    owners, groups = lax.axis_size("tbl"), lax.axis_size("grp")
    batch = ids.shape[0]
    slots, rows = tables.shape[:2]
    maxlen = ids.shape[1] // (slots * owners)
    factor = 1.0 / math.sqrt(batch * owners * groups)
    tiled = by_exchange(owners, groups, *down.shape)

    if tiled:
        masked, own = prep(slot_of_table, ids, lengths, x, ct, down, up, maxlen, rows)
        keep, came = exchange_start(x, ct, own)
    else:
        masked = mask_ids(slot_of_table, ids, lengths, maxlen, rows)
    got = lax.all_to_all(masked.reshape(owners, slots * maxlen, batch), "tbl", 0, 0)
    if tiled:
        got, keep = lax.optimization_barrier((got, keep))
    firsts, counts = (0,), (slots,)
    parts = []
    for first, count in zip(firsts, counts):
        pooled = pool_slots(got, tables, first, count, maxlen)
        parts.append(lax.all_to_all(pooled, "tbl", 0, 0))
    embedded = place(slot_of_table, parts, firsts, counts, slots)
    if tiled:
        grad_up, grad_down = exchange_end(keep, came, factor)
    else:
        grad_up, grad_down = grads_plain(x, ct, up, down, factor)
    return embedded, grad_up, grad_down


def by_exchange(owners, groups, wide, rank):
    each, part = wide // groups, rank // owners
    return owners % 2 == 0 and groups % 2 == 0 and each % 16 == 0 and 2 * part % LANES == 0


def solution(mesh):
    rows = P(("grp", "tbl"), None)
    return jax.shard_map(
        on_device,
        mesh=mesh,
        in_specs=(rows, rows, P(), P("tbl", None, None), rows, rows, P(), P()),
        out_specs=(rows, P("tbl", "grp"), P("grp", "tbl")),
        check_vma=False,
    )
```

```python
import functools
import math

import jax
import jax.numpy as jnp
from jax import lax
from jax.experimental import pallas as pl
from jax.experimental.pallas import tpu as pltpu
from jax.sharding import PartitionSpec as P


F32 = jnp.float32
BF16 = jnp.bfloat16
LANES = 128


def room(mebibytes):
    return pltpu.CompilerParams(vmem_limit_bytes=mebibytes * 2**20)


def whole(memory=pltpu.VMEM):
    return pl.BlockSpec(memory_space=memory)


def in_hbm(x):
    return pltpu.with_memory_space_constraint(x, pltpu.HBM)


def masked_ids(slot_ref, ids_ref, lens_ref, maxlen, rows):
    entries, batch = ids_ref.shape
    feats = lens_ref.shape[0]
    slot_of_row = lax.broadcasted_iota(jnp.int32, (entries, feats), 0) // maxlen
    hit = (slot_of_row == slot_ref[...]).astype(F32)
    lens = jnp.dot(hit, lens_ref[...].astype(F32), preferred_element_type=F32)
    place = lax.broadcasted_iota(jnp.int32, (entries, batch), 0) % maxlen
    keep = place.astype(F32) + 0.5 < lens
    return jnp.where(keep, ids_ref[...], rows)


def mask_kernel(slot_ref, ids_ref, lens_ref, out_ref, *, maxlen, rows):
    out_ref[...] = masked_ids(slot_ref, ids_ref, lens_ref, maxlen, rows)


def mask_ids(slot_of_table, ids, lengths, maxlen, rows):
    return pl.pallas_call(
        functools.partial(mask_kernel, maxlen=maxlen, rows=rows),
        in_specs=[whole()] * 3,
        out_specs=whole(),
        out_shape=jax.ShapeDtypeStruct((ids.shape[1], ids.shape[0]), jnp.int32),
        compiler_params=room(4),
        name="mask_ids",
    )(slot_of_table.reshape(1, -1), ids.T, lengths.T)


def prep_kernel(*refs, maxlen, rows):
    sources, (masked_ref, rank_ref), targets, sem = refs[:7], refs[7:9], refs[9:16], refs[16]
    slot_ref, ids_ref, lens_ref, x_ref, ct_ref, down_ref, up_ref = targets
    loads = [
        pltpu.make_async_copy(src, dst, sem.at[i]) for i, (src, dst) in enumerate(zip(sources, targets))
    ]
    for load in loads:
        load.start()
    for load in loads[:3]:
        load.wait()
    masked_ref[...] = masked_ids(slot_ref, ids_ref, lens_ref, maxlen, rows)
    for load in loads[3:5]:
        load.wait()
    x = x_ref[...]
    dz = (ct_ref[...].astype(F32) * x.astype(F32)).astype(BF16)
    loads[5].wait()
    rank_ref[0] = jnp.dot(x, down_ref[...], preferred_element_type=F32).astype(BF16)
    loads[6].wait()
    rank_ref[1] = lax.dot_general(
        dz, up_ref[...], (((1,), (1,)), ((), ())), preferred_element_type=F32
    ).astype(BF16)


def prep(slot_of_table, ids, lengths, x, ct, down, up, maxlen, rows):
    sources = [slot_of_table.reshape(1, -1), ids.T, lengths.T, x, ct, down, up]
    return pl.pallas_call(
        functools.partial(prep_kernel, maxlen=maxlen, rows=rows),
        in_specs=[whole(pl.ANY)] * 7,
        out_specs=[whole()] * 2,
        out_shape=[
            jax.ShapeDtypeStruct(ids.shape[::-1], jnp.int32),
            jax.ShapeDtypeStruct((2, x.shape[0], down.shape[1]), BF16),
        ],
        scratch_shapes=[pltpu.VMEM(a.shape, a.dtype) for a in sources]
        + [pltpu.SemaphoreType.DMA((7,))],
        compiler_params=room(16),
        name="prep",
    )(*[in_hbm(a) for a in sources])


def pool_kernel(ids_hbm, tables_hbm, out_hbm, *refs, maxlen):
    groups, count, batch, width = out_hbm.shape
    near, refs = refs[:groups], refs[groups:]
    stage, wide, pooled, sum_ref = refs[0:2], refs[2:4], refs[4:6], refs[6]
    ids_sem, first_sem, table_sem, out_sem = refs[7:]
    rows = stage[0].shape[0]
    firsts = first_sem.shape[0]
    head = rows // firsts
    piece = math.gcd(rows, 48)
    pieces = rows // piece

    def fetch_ids(g, slot):
        start = pl.multiple_of(slot * maxlen, maxlen)
        return pltpu.make_async_copy(ids_hbm.at[g, pl.ds(start, maxlen)], near[g], ids_sem.at[g])

    def fetch_table(slot, at):
        return pltpu.make_async_copy(tables_hbm.at[slot], stage[at], table_sem.at[at])

    def fetch_first(i):
        part = pl.ds(i * head, head)
        return pltpu.make_async_copy(tables_hbm.at[0, part], stage[0].at[part], first_sem.at[i])

    def put(slot, at):
        return pltpu.make_async_copy(pooled[at], out_hbm.at[:, slot], out_sem.at[at])

    def widen(at, start, size):
        part = pl.ds(start, size)
        wide[at][part, :] = stage[at][part, :].astype(F32)

    def half(slot, at):
        other = 1 - at

        @pl.when(slot + 1 < count)
        def _():
            fetch_table(slot + 1, other).wait()

        @pl.when(slot + 2 < count)
        def _():
            fetch_table(slot + 2, at).start()

        @pl.when(slot >= 2)
        def _():
            put(slot - 2, at).wait()

        for g in range(groups):
            fetch_ids(g, slot).wait()
            for b in range(batch):
                bag = g * batch + b
                for p in range(bag * pieces // (groups * batch), (bag + 1) * pieces // (groups * batch)):
                    widen(other, p * piece, piece)
                total = wide[at][pl.ds(near[g][0, b], 1), :]
                for k in range(1, maxlen):
                    total = total + wide[at][pl.ds(near[g][k, b], 1), :]
                sum_ref[pl.ds(b, 1), :] = total
            pooled[at][g] = sum_ref[...].astype(BF16)

            @pl.when(slot + 1 < count)
            def _(g=g):
                fetch_ids(g, slot + 1).start()

        put(slot, at).start()

    for g in range(groups):
        fetch_ids(g, 0).start()
    for i in range(firsts):
        fetch_first(i).start()
    if count > 1:
        fetch_table(1, 1).start()
    for at in range(2):
        wide[at][pl.ds(rows, 8), :] = jnp.zeros((8, width), F32)
    for i in range(firsts):
        fetch_first(i).wait()
        widen(0, i * head, head)

    def pair(i, carry):
        half(2 * i, 0)

        @pl.when(2 * i + 1 < count)
        def _():
            half(2 * i + 1, 1)

        return carry

    lax.fori_loop(0, (count + 1) // 2, pair, 0)
    for slot in range(max(count - 2, 0), count):
        put(slot, slot % 2).wait()


def pool_slots(ids, tables, maxlen):
    groups, _, batch = ids.shape
    slots, rows, width = tables.shape
    firsts = 4 if rows % 64 == 0 else 1
    return pl.pallas_call(
        functools.partial(pool_kernel, maxlen=maxlen),
        in_specs=[whole(pl.ANY)] * 2,
        out_specs=whole(pl.ANY),
        out_shape=jax.ShapeDtypeStruct((groups, slots, batch, width), BF16),
        scratch_shapes=[pltpu.SMEM((maxlen, batch), jnp.int32)] * groups
        + [pltpu.VMEM((rows, width), BF16)] * 2
        + [pltpu.VMEM((rows + 8, width), F32)] * 2
        + [pltpu.VMEM((groups, batch, width), BF16)] * 2
        + [pltpu.VMEM((batch, width), F32)]
        + [pltpu.SemaphoreType.DMA((n,)) for n in (groups, firsts, 2, 2)],
        compiler_params=room(16),
        name="pool_slots",
    )(ids, in_hbm(tables))


def place_kernel(slot_ref, pooled_ref, out_ref, sem):
    slots, _, width = pooled_ref.shape[1:]
    feats = slot_ref.shape[0]

    def put(f, slot):
        owner = lax.div(slot, slots)
        to = out_ref.at[:, pl.ds(f * width, width)]
        return pltpu.make_async_copy(pooled_ref.at[owner, slot - owner * slots], to, sem.at[f])

    for f in range(feats):
        put(f, slot_ref[f]).start()
    for f in range(feats):
        put(f, slot_ref[f]).wait()


def place(slot_of_table, pooled):
    batch, width = pooled.shape[2:]
    feats = slot_of_table.shape[0]
    return pl.pallas_call(
        place_kernel,
        in_specs=[whole(pltpu.SMEM), whole(pl.ANY)],
        out_specs=whole(pl.ANY),
        out_shape=jax.ShapeDtypeStruct((batch, feats * width), BF16),
        scratch_shapes=[pltpu.SemaphoreType.DMA((feats,))],
        compiler_params=room(4),
        name="place",
    )(slot_of_table, pooled)


def grads_kernel(pos_ref, own_ref, sib_ref, *refs, owners, groups, chunks):
    tall, far = owners // 2, groups // 2
    sources, keep_ref, sends = refs[:4], refs[4], refs[5 : 4 + 2 * tall]
    both_ref, sum_ref, near_ref, in_sem, sem = refs[4 + 2 * tall : 9 + 2 * tall]
    targets = refs[9 + 2 * tall :]
    g, t = lax.div(pos_ref[0], owners), lax.rem(pos_ref[0], owners)
    core, y, x, z = t & 1, t >> 1, g & 1, g >> 1
    batch, wide = sources[0].shape
    part = own_ref.shape[2] // owners
    pair = 2 * batch
    span = wide // chunks
    loads = []
    for c in range(chunks):
        at = pl.ds(c * span, span)
        loads.append(
            [
                pltpu.make_async_copy(src.at[:, at], dst.at[:, at], in_sem.at[4 * c + i])
                for i, (src, dst) in enumerate(zip(sources, targets))
            ]
        )
        for load in loads[-1]:
            load.start()
    low = jnp.concatenate([own_ref[0], sib_ref[0]], axis=0).astype(F32)
    dlow = jnp.concatenate([own_ref[1], sib_ref[1]], axis=0).astype(F32)
    none = jnp.zeros((pair, part), F32)
    columns = []
    for ry in range(tall):
        owner = 2 * lax.rem(y + ry, tall) + core
        lo, dl = none, none
        for t in range(owners):
            lo = jnp.where(owner == t, low[:, t * part : (t + 1) * part], lo)
            dl = jnp.where(owner == t, dlow[:, t * part : (t + 1) * part], dl)
        columns.append(
            jnp.concatenate(
                [jnp.concatenate([lo, none], axis=1), jnp.concatenate([none, dl], axis=1)], axis=0
            )
        )
    right = jnp.concatenate(columns, axis=1).astype(BF16)
    step = math.gcd(span, 384)
    for c in range(chunks):
        for load in loads[c]:
            load.wait()
        for d in range(c * span, (c + 1) * span, step):
            cols = slice(d, d + step)
            for i in range(2):
                a = targets[2 * i][:, cols]
                dz = targets[2 * i + 1][:, cols].astype(F32) * a.astype(F32)
                both_ref[pl.ds(i * batch, batch), :] = dz.astype(BF16)
                both_ref[pl.ds(pair + i * batch, batch), :] = a
            sum_ref[pl.ds(d, step), :] = lax.dot_general(
                both_ref[...], right, (((0,), (0,)), ((), ())), preferred_element_type=F32
            )
    each = wide // groups
    block = 2 * part
    copies = []
    for i in range(2 * tall - 1, -1, -1):
        rx, ry = i // tall, i % tall
        cols = slice(ry * block, (ry + 1) * block)
        for r in range(far):
            g = 2 * lax.rem(z + r, far) + (x + rx - 2 * x * rx)
            found = sum_ref[pl.ds(pl.multiple_of(g * each, 16), each), cols]
            if i:
                near_ref[i - 1, r] = found.astype(BF16)
            else:
                keep_ref[r] = found
        if i:
            copies.append(pltpu.make_async_copy(near_ref.at[i - 1], sends[i - 1], sem.at[i - 1]))
            copies[-1].start()
    for copy in copies:
        copy.wait()


def part_grads(pos, own, sib, x, ct, xs, cts, owners, groups):
    batch, wide = x.shape
    rank = own.shape[2]
    tall, far = owners // 2, groups // 2
    block = 2 * (rank // owners)
    shape = (far, wide // groups, block)
    others = 2 * tall - 1
    chunks = 3 if wide % (3 * LANES) == 0 else 1
    step = math.gcd(wide // chunks, 384)
    return pl.pallas_call(
        functools.partial(grads_kernel, owners=owners, groups=groups, chunks=chunks),
        in_specs=[whole(pltpu.SMEM)] + [whole()] * 2 + [whole(pl.ANY)] * 4,
        out_specs=[whole()] + [whole(pltpu.HBM)] * others,
        out_shape=[jax.ShapeDtypeStruct(shape, F32)] + [pltpu.HBM(shape, BF16)] * others,
        scratch_shapes=[
            pltpu.VMEM((4 * batch, step), BF16),
            pltpu.VMEM((wide, tall * block), F32),
            pltpu.VMEM((others, *shape), BF16),
            pltpu.SemaphoreType.DMA((4 * chunks,)),
            pltpu.SemaphoreType.DMA((others,)),
        ]
        + [pltpu.VMEM((batch, wide), BF16)] * 4,
        compiler_params=room(20),
        name="part_grads",
    )(pos, own, sib, in_hbm(x), in_hbm(ct), xs, cts)


def fold_kernel(keep, *refs, far):
    came, outs = refs[:-far], refs[-far:]
    for r in range(far):
        total = keep[r]
        for one in came:
            total = total + one[r].astype(F32)
        outs[r][...] = total.astype(outs[r].dtype)


def fold(keep, came):
    far, rows, block = keep.shape
    return pl.pallas_call(
        functools.partial(fold_kernel, far=far),
        in_specs=[whole()] * (1 + len(came)),
        out_specs=[whole()] * far,
        out_shape=[jax.ShapeDtypeStruct((rows, block), BF16 if r else F32) for r in range(far)],
        compiler_params=room(12),
        name="fold",
    )(keep, *came)


def finish_kernel(*refs, factor):
    up_ref, down_ref = refs[-2:]
    total = refs[0][...]
    for r in refs[1:-2]:
        total = total + r[...].astype(F32)
    total = total * factor
    half = total.shape[1] // 2
    flat = total.T
    up_ref[...] = flat[:half, :]
    down_ref[...] = flat[half:, :]


def finish(keep, came, factor):
    rows, block = keep.shape
    half = block // 2
    shape = jax.ShapeDtypeStruct
    up, down = pl.pallas_call(
        functools.partial(finish_kernel, factor=factor),
        in_specs=[whole()] * (1 + len(came)),
        out_specs=[whole()] * 2,
        out_shape=[shape((half, rows), F32)] * 2,
        compiler_params=room(8),
        name="finish",
    )(keep, *came)
    return up, down.T


def exchange_start(x, ct, own):
    owners, groups = lax.axis_size("tbl"), lax.axis_size("grp")
    tall = owners // 2
    pos = lax.axis_index(("grp", "tbl")).astype(jnp.int32).reshape(1)
    other_core = [(i, i ^ 1) for i in range(owners)]
    xs = lax.ppermute(x, "tbl", other_core)
    cts = lax.ppermute(ct, "tbl", other_core)
    sib = lax.ppermute(own, "tbl", other_core)
    parts = part_grads(pos, own, sib, x, ct, xs, cts, owners, groups)

    def to(rx, ry):
        return [
            (i * owners + j, (i ^ rx) * owners + 2 * ((j // 2 + ry) % tall) + j % 2)
            for i in range(groups)
            for j in range(owners)
        ]

    came = []
    for i in range(1, 2 * tall):
        came.append(lax.ppermute(parts[i], ("grp", "tbl"), to(i // tall, i % tall)))
    return parts[0], came


def exchange_end(keep, came, embedded, factor):
    groups = lax.axis_size("grp")
    far = groups // 2

    def to_z(r):
        return [(i, 2 * ((i // 2 + r) % far) + i % 2) for i in range(groups)]

    out = fold(keep, came)
    last = []
    for r in range(1, far):
        last.append(lax.ppermute(out[r], "grp", to_z(r)))
    embedded, keep = lax.optimization_barrier((embedded, out[0]))
    return embedded, *finish(keep, last, factor)


def grads_plain(x, ct, up, down, factor):
    low = jnp.dot(x, down, preferred_element_type=F32).astype(BF16)
    dz = (ct.astype(F32) * x.astype(F32)).astype(BF16)
    dlow = jnp.dot(dz, up.T, preferred_element_type=F32).astype(BF16)
    part_up = jnp.dot(low.T, dz, preferred_element_type=F32) * factor
    part_down = jnp.dot(x.T, dlow, preferred_element_type=F32) * factor
    owner_up = lax.psum_scatter(part_up, "tbl", scatter_dimension=0, tiled=True)
    owner_down = lax.psum_scatter(part_down, "tbl", scatter_dimension=1, tiled=True)
    return (
        lax.psum_scatter(owner_up, "grp", scatter_dimension=1, tiled=True),
        lax.psum_scatter(owner_down, "grp", scatter_dimension=0, tiled=True),
    )


def on_device(ids, lengths, slot_of_table, tables, x, ct, up, down):
    owners, groups = lax.axis_size("tbl"), lax.axis_size("grp")
    batch = ids.shape[0]
    slots, rows = tables.shape[:2]
    maxlen = ids.shape[1] // (slots * owners)
    factor = 1.0 / math.sqrt(batch * owners * groups)
    tiled = by_exchange(owners, groups, *down.shape)

    if tiled:
        masked, own = prep(slot_of_table, ids, lengths, x, ct, down, up, maxlen, rows)
        keep, came = exchange_start(x, ct, own)
    else:
        masked = mask_ids(slot_of_table, ids, lengths, maxlen, rows)
    got = lax.all_to_all(masked.reshape(owners, slots * maxlen, batch), "tbl", 0, 0)
    if tiled:
        got, keep = lax.optimization_barrier((got, keep))
    pooled = pool_slots(got, tables, maxlen)
    pooled = lax.all_to_all(pooled, "tbl", 0, 0)
    embedded = place(slot_of_table, pooled)
    if tiled:
        embedded, grad_up, grad_down = exchange_end(keep, came, embedded, factor)
    else:
        grad_up, grad_down = grads_plain(x, ct, up, down, factor)
    return embedded, grad_up, grad_down


def by_exchange(owners, groups, wide, rank):
    each, part = wide // groups, rank // owners
    return owners % 2 == 0 and groups % 2 == 0 and each % 16 == 0 and 2 * part % LANES == 0


def solution(mesh):
    rows = P(("grp", "tbl"), None)
    return jax.shard_map(
        on_device,
        mesh=mesh,
        in_specs=(rows, rows, P(), P("tbl", None, None), rows, rows, P(), P()),
        out_specs=(rows, P("tbl", "grp"), P("grp", "tbl")),
        check_vma=False,
    )
```

```python
import functools
import math

import jax
import jax.numpy as jnp
from jax import lax
from jax.experimental import pallas as pl
from jax.experimental.pallas import tpu as pltpu
from jax.sharding import PartitionSpec as P


F32 = jnp.float32
BF16 = jnp.bfloat16
LANES = 128


def room(mebibytes):
    return pltpu.CompilerParams(vmem_limit_bytes=mebibytes * 2**20)


def whole(memory=pltpu.VMEM):
    return pl.BlockSpec(memory_space=memory)


def in_hbm(x):
    return pltpu.with_memory_space_constraint(x, pltpu.HBM)


def owner_at(t, d, owners):
    return 2 * lax.rem((t >> 1) + (d >> 1), owners // 2) + ((t & 1) ^ (d & 1))


def owner_pairs(d, owners):
    return [(t, 2 * ((t // 2 + d // 2) % (owners // 2)) + (t % 2 ^ d % 2)) for t in range(owners)]


def masked_ids(slot_ref, ids_ref, lens_ref, maxlen, rows):
    entries, batch = ids_ref.shape
    feats = lens_ref.shape[0]
    slot_of_row = lax.broadcasted_iota(jnp.int32, (entries, feats), 0) // maxlen
    hit = (slot_of_row == slot_ref[...]).astype(F32)
    lens = jnp.dot(hit, lens_ref[...].astype(F32), preferred_element_type=F32)
    place = lax.broadcasted_iota(jnp.int32, (entries, batch), 0) % maxlen
    keep = place.astype(F32) + 0.5 < lens
    return jnp.where(keep, ids_ref[...], rows)


def prep_kernel(pos_ref, *refs, owners, maxlen, rows):
    sources, mine, rank_ref = refs[:7], refs[7 : 7 + owners], refs[7 + owners]
    targets, masked_ref, sem = refs[8 + owners : 15 + owners], refs[15 + owners], refs[16 + owners]
    slot_ref, ids_ref, lens_ref, x_ref, ct_ref, down_ref, up_ref = targets
    loads = [
        pltpu.make_async_copy(src, dst, sem.at[i]) for i, (src, dst) in enumerate(zip(sources, targets))
    ]
    for load in loads:
        load.start()
    for load in loads[:3]:
        load.wait()
    masked_ref[...] = masked_ids(slot_ref, ids_ref, lens_ref, maxlen, rows)
    t = lax.rem(pos_ref[0], owners)
    entries = mine[0].shape[0]
    for d in range(owners):
        start = pl.multiple_of(owner_at(t, d, owners) * entries, maxlen)
        mine[d][...] = masked_ref[pl.ds(start, entries), :]
    for load in loads[3:5]:
        load.wait()
    x = x_ref[...]
    dz = (ct_ref[...].astype(F32) * x.astype(F32)).astype(BF16)
    loads[5].wait()
    rank_ref[0] = jnp.dot(x, down_ref[...], preferred_element_type=F32).astype(BF16)
    loads[6].wait()
    rank_ref[1] = lax.dot_general(
        dz, up_ref[...], (((1,), (1,)), ((), ())), preferred_element_type=F32
    ).astype(BF16)


def prep(pos, slot_of_table, ids, lengths, x, ct, down, up, owners, maxlen, rows):
    sources = [slot_of_table.reshape(1, -1), ids.T, lengths.T, x, ct, down, up]
    batch, entries = ids.shape
    *mine, rank = pl.pallas_call(
        functools.partial(prep_kernel, owners=owners, maxlen=maxlen, rows=rows),
        in_specs=[whole(pltpu.SMEM)] + [whole(pl.ANY)] * 7,
        out_specs=[whole()] * (owners + 1),
        out_shape=[jax.ShapeDtypeStruct((entries // owners, batch), jnp.int32)] * owners
        + [jax.ShapeDtypeStruct((2, batch, down.shape[1]), BF16)],
        scratch_shapes=[pltpu.VMEM(a.shape, a.dtype) for a in sources]
        + [pltpu.VMEM((entries, batch), jnp.int32), pltpu.SemaphoreType.DMA((7,))],
        compiler_params=room(16),
        name="prep",
    )(pos, *[in_hbm(a) for a in sources])
    return mine, rank


def pool_kernel(*refs, groups, maxlen):
    ids_hbm, tables_hbm, outs = refs[:groups], refs[groups], refs[groups + 1 : 2 * groups + 1]
    near, refs = refs[2 * groups + 1 : 3 * groups + 1], refs[3 * groups + 1 :]
    count, batch, width = outs[0].shape
    stage, wide, pooled, sum_ref = refs[0:2], refs[2:4], refs[4:6], refs[6]
    ids_sem, first_sem, table_sem, out_sem = refs[7:]
    rows = stage[0].shape[0]
    firsts = first_sem.shape[0]
    head = rows // firsts
    piece = math.gcd(rows, 48)
    pieces = rows // piece

    def fetch_ids(g, slot):
        start = pl.multiple_of(slot * maxlen, maxlen)
        return pltpu.make_async_copy(ids_hbm[g].at[pl.ds(start, maxlen)], near[g], ids_sem.at[g])

    def fetch_table(slot, at):
        return pltpu.make_async_copy(tables_hbm.at[slot], stage[at], table_sem.at[at])

    def fetch_first(i):
        part = pl.ds(i * head, head)
        return pltpu.make_async_copy(tables_hbm.at[0, part], stage[0].at[part], first_sem.at[i])

    def put(slot, at, g):
        return pltpu.make_async_copy(pooled[at].at[g], outs[g].at[slot], out_sem.at[at * groups + g])

    def widen(at, start, size):
        part = pl.ds(start, size)
        wide[at][part, :] = stage[at][part, :].astype(F32)

    def half(slot, at):
        other = 1 - at

        @pl.when(slot + 1 < count)
        def _():
            fetch_table(slot + 1, other).wait()

        @pl.when(slot + 2 < count)
        def _():
            fetch_table(slot + 2, at).start()

        @pl.when(slot >= 2)
        def _():
            for g in range(groups):
                put(slot - 2, at, g).wait()

        for g in range(groups):
            fetch_ids(g, slot).wait()
            for b in range(batch):
                bag = g * batch + b
                for p in range(bag * pieces // (groups * batch), (bag + 1) * pieces // (groups * batch)):
                    widen(other, p * piece, piece)
                total = wide[at][pl.ds(near[g][0, b], 1), :]
                for k in range(1, maxlen):
                    total = total + wide[at][pl.ds(near[g][k, b], 1), :]
                sum_ref[pl.ds(b, 1), :] = total
            pooled[at][g] = sum_ref[...].astype(BF16)
            put(slot, at, g).start()

            @pl.when(slot + 1 < count)
            def _(g=g):
                fetch_ids(g, slot + 1).start()

    for g in range(groups):
        fetch_ids(g, 0).start()
    for i in range(firsts):
        fetch_first(i).start()
    if count > 1:
        fetch_table(1, 1).start()
    for at in range(2):
        wide[at][pl.ds(rows, 8), :] = jnp.zeros((8, width), F32)
    for i in range(firsts):
        fetch_first(i).wait()
        widen(0, i * head, head)

    def pair(i, carry):
        half(2 * i, 0)

        @pl.when(2 * i + 1 < count)
        def _():
            half(2 * i + 1, 1)

        return carry

    lax.fori_loop(0, (count + 1) // 2, pair, 0)
    for slot in range(max(count - 2, 0), count):
        for g in range(groups):
            put(slot, slot % 2, g).wait()


def pool_slots(ids, tables, maxlen):
    groups, batch = len(ids), ids[0].shape[1]
    slots, rows, width = tables.shape
    firsts = 4 if rows % 64 == 0 else 1
    return pl.pallas_call(
        functools.partial(pool_kernel, groups=groups, maxlen=maxlen),
        in_specs=[whole(pl.ANY)] * (groups + 1),
        out_specs=[whole(pl.ANY)] * groups,
        out_shape=[jax.ShapeDtypeStruct((slots, batch, width), BF16)] * groups,
        scratch_shapes=[pltpu.SMEM((maxlen, batch), jnp.int32)] * groups
        + [pltpu.VMEM((rows, width), BF16)] * 2
        + [pltpu.VMEM((rows + 8, width), F32)] * 2
        + [pltpu.VMEM((groups, batch, width), BF16)] * 2
        + [pltpu.VMEM((batch, width), F32)]
        + [pltpu.SemaphoreType.DMA((n,)) for n in (groups, firsts, 2, 2 * groups)],
        compiler_params=room(16),
        name="pool_slots",
    )(*ids, in_hbm(tables))


def place_kernel(pos_ref, slot_ref, *refs):
    parts, out_ref, sem = refs[:-2], refs[-2], refs[-1]
    owners = len(parts)
    slots, _, width = parts[0].shape
    feats = slot_ref.shape[0]
    t = lax.rem(pos_ref[0], owners)

    def put(f, part, local):
        to = out_ref.at[:, pl.ds(f * width, width)]
        return pltpu.make_async_copy(part.at[local], to, sem.at[f])

    for d, part in enumerate(parts):
        first = owner_at(t, d, owners) * slots
        for f in range(feats):
            local = slot_ref[f] - first

            @pl.when((local >= 0) & (local < slots))
            def _(f=f, part=part, local=local):
                put(f, part, local).start()

    for f in range(feats):
        put(f, parts[0], 0).wait()


def place(pos, slot_of_table, parts):
    _, batch, width = parts[0].shape
    feats = slot_of_table.shape[0]
    return pl.pallas_call(
        place_kernel,
        in_specs=[whole(pltpu.SMEM)] * 2 + [whole(pl.ANY)] * len(parts),
        out_specs=whole(pl.ANY),
        out_shape=jax.ShapeDtypeStruct((batch, feats * width), BF16),
        scratch_shapes=[pltpu.SemaphoreType.DMA((feats,))],
        compiler_params=room(4),
        name="place",
    )(pos, slot_of_table, *parts)


def grads_kernel(pos_ref, own_ref, sib_ref, *refs, owners, groups, chunks):
    tall, far = owners // 2, groups // 2
    sources, keep_ref, sends = refs[:4], refs[4], refs[5 : 4 + 2 * tall]
    both_ref, sum_ref, near_ref, in_sem, sem = refs[4 + 2 * tall : 9 + 2 * tall]
    targets = refs[9 + 2 * tall :]
    g, t = lax.div(pos_ref[0], owners), lax.rem(pos_ref[0], owners)
    core, y, x, z = t & 1, t >> 1, g & 1, g >> 1
    batch, wide = sources[0].shape
    part = own_ref.shape[2] // owners
    pair = 2 * batch
    span = wide // chunks
    loads = []
    for c in range(chunks):
        at = pl.ds(c * span, span)
        loads.append(
            [
                pltpu.make_async_copy(src.at[:, at], dst.at[:, at], in_sem.at[4 * c + i])
                for i, (src, dst) in enumerate(zip(sources, targets))
            ]
        )
        for load in loads[-1]:
            load.start()
    low = jnp.concatenate([own_ref[0], sib_ref[0]], axis=0).astype(F32)
    dlow = jnp.concatenate([own_ref[1], sib_ref[1]], axis=0).astype(F32)
    none = jnp.zeros((pair, part), F32)
    columns = []
    for ry in range(tall):
        owner = 2 * lax.rem(y + ry, tall) + core
        lo, dl = none, none
        for t in range(owners):
            lo = jnp.where(owner == t, low[:, t * part : (t + 1) * part], lo)
            dl = jnp.where(owner == t, dlow[:, t * part : (t + 1) * part], dl)
        columns.append(
            jnp.concatenate(
                [jnp.concatenate([lo, none], axis=1), jnp.concatenate([none, dl], axis=1)], axis=0
            )
        )
    right = jnp.concatenate(columns, axis=1).astype(BF16)
    step = math.gcd(span, 384)
    for c in range(chunks):
        for load in loads[c]:
            load.wait()
        for d in range(c * span, (c + 1) * span, step):
            cols = slice(d, d + step)
            for i in range(2):
                a = targets[2 * i][:, cols]
                dz = targets[2 * i + 1][:, cols].astype(F32) * a.astype(F32)
                both_ref[pl.ds(i * batch, batch), :] = dz.astype(BF16)
                both_ref[pl.ds(pair + i * batch, batch), :] = a
            sum_ref[pl.ds(d, step), :] = lax.dot_general(
                both_ref[...], right, (((0,), (0,)), ((), ())), preferred_element_type=F32
            )
    each = wide // groups
    block = 2 * part
    copies = []
    for i in range(2 * tall - 1, -1, -1):
        rx, ry = i // tall, i % tall
        cols = slice(ry * block, (ry + 1) * block)
        for r in range(far):
            g = 2 * lax.rem(z + r, far) + (x + rx - 2 * x * rx)
            found = sum_ref[pl.ds(pl.multiple_of(g * each, 16), each), cols]
            if i:
                near_ref[i - 1, r] = found.astype(BF16)
            else:
                keep_ref[r] = found
        if i:
            copies.append(pltpu.make_async_copy(near_ref.at[i - 1], sends[i - 1], sem.at[i - 1]))
            copies[-1].start()
    for copy in copies:
        copy.wait()


def part_grads(pos, own, sib, x, ct, xs, cts, owners, groups):
    batch, wide = x.shape
    rank = own.shape[2]
    tall, far = owners // 2, groups // 2
    block = 2 * (rank // owners)
    shape = (far, wide // groups, block)
    others = 2 * tall - 1
    chunks = 3 if wide % (3 * LANES) == 0 else 1
    step = math.gcd(wide // chunks, 384)
    return pl.pallas_call(
        functools.partial(grads_kernel, owners=owners, groups=groups, chunks=chunks),
        in_specs=[whole(pltpu.SMEM)] + [whole()] * 2 + [whole(pl.ANY)] * 4,
        out_specs=[whole()] + [whole(pltpu.HBM)] * others,
        out_shape=[jax.ShapeDtypeStruct(shape, F32)] + [pltpu.HBM(shape, BF16)] * others,
        scratch_shapes=[
            pltpu.VMEM((4 * batch, step), BF16),
            pltpu.VMEM((wide, tall * block), F32),
            pltpu.VMEM((others, *shape), BF16),
            pltpu.SemaphoreType.DMA((4 * chunks,)),
            pltpu.SemaphoreType.DMA((others,)),
        ]
        + [pltpu.VMEM((batch, wide), BF16)] * 4,
        compiler_params=room(20),
        name="part_grads",
    )(pos, own, sib, in_hbm(x), in_hbm(ct), xs, cts)


def fold_kernel(keep, *refs, far):
    came, outs = refs[:-far], refs[-far:]
    for r in range(far):
        total = keep[r]
        for one in came:
            total = total + one[r].astype(F32)
        outs[r][...] = total.astype(outs[r].dtype)


def fold(keep, came):
    far, rows, block = keep.shape
    return pl.pallas_call(
        functools.partial(fold_kernel, far=far),
        in_specs=[whole()] * (1 + len(came)),
        out_specs=[whole()] * far,
        out_shape=[jax.ShapeDtypeStruct((rows, block), BF16 if r else F32) for r in range(far)],
        compiler_params=room(12),
        name="fold",
    )(keep, *came)


def finish_kernel(*refs, factor):
    up_ref, down_ref = refs[-2:]
    total = refs[0][...]
    for r in refs[1:-2]:
        total = total + r[...].astype(F32)
    total = total * factor
    half = total.shape[1] // 2
    flat = total.T
    up_ref[...] = flat[:half, :]
    down_ref[...] = flat[half:, :]


def finish(keep, came, factor):
    rows, block = keep.shape
    half = block // 2
    shape = jax.ShapeDtypeStruct
    up, down = pl.pallas_call(
        functools.partial(finish_kernel, factor=factor),
        in_specs=[whole()] * (1 + len(came)),
        out_specs=[whole()] * 2,
        out_shape=[shape((half, rows), F32)] * 2,
        compiler_params=room(8),
        name="finish",
    )(keep, *came)
    return up, down.T


def exchange_start(pos, x, ct, own):
    owners, groups = lax.axis_size("tbl"), lax.axis_size("grp")
    tall = owners // 2
    other_core = [(i, i ^ 1) for i in range(owners)]
    xs = lax.ppermute(x, "tbl", other_core)
    cts = lax.ppermute(ct, "tbl", other_core)
    sib = lax.ppermute(own, "tbl", other_core)
    parts = part_grads(pos, own, sib, x, ct, xs, cts, owners, groups)

    def to(rx, ry):
        return [
            (i * owners + j, (i ^ rx) * owners + 2 * ((j // 2 + ry) % tall) + j % 2)
            for i in range(groups)
            for j in range(owners)
        ]

    came = []
    for i in range(1, 2 * tall):
        came.append(lax.ppermute(parts[i], ("grp", "tbl"), to(i // tall, i % tall)))
    return parts[0], came


def exchange_end(keep, came, embedded, factor):
    groups = lax.axis_size("grp")
    far = groups // 2

    def to_z(r):
        return [(i, 2 * ((i // 2 + r) % far) + i % 2) for i in range(groups)]

    out = fold(keep, came)
    last = []
    for r in range(1, far):
        last.append(lax.ppermute(out[r], "grp", to_z(r)))
    embedded, keep = lax.optimization_barrier((embedded, out[0]))
    return embedded, *finish(keep, last, factor)


def grads_plain(x, ct, up, down, factor):
    low = jnp.dot(x, down, preferred_element_type=F32).astype(BF16)
    dz = (ct.astype(F32) * x.astype(F32)).astype(BF16)
    dlow = jnp.dot(dz, up.T, preferred_element_type=F32).astype(BF16)
    part_up = jnp.dot(low.T, dz, preferred_element_type=F32) * factor
    part_down = jnp.dot(x.T, dlow, preferred_element_type=F32) * factor
    owner_up = lax.psum_scatter(part_up, "tbl", scatter_dimension=0, tiled=True)
    owner_down = lax.psum_scatter(part_down, "tbl", scatter_dimension=1, tiled=True)
    return (
        lax.psum_scatter(owner_up, "grp", scatter_dimension=1, tiled=True),
        lax.psum_scatter(owner_down, "grp", scatter_dimension=0, tiled=True),
    )


def on_device(ids, lengths, slot_of_table, tables, x, ct, up, down):
    owners, groups = lax.axis_size("tbl"), lax.axis_size("grp")
    batch = ids.shape[0]
    slots, rows = tables.shape[:2]
    maxlen = ids.shape[1] // (slots * owners)
    factor = 1.0 / math.sqrt(batch * owners * groups)
    tiled = by_exchange(owners, groups, *down.shape)

    pos = lax.axis_index(("grp", "tbl")).astype(jnp.int32).reshape(1)
    mine, own = prep(pos, slot_of_table, ids, lengths, x, ct, down, up, owners, maxlen, rows)
    got = list(mine[:1])
    for d in range(1, owners):
        got.append(lax.ppermute(mine[d], "tbl", owner_pairs(d, owners)))
    if tiled:
        keep, came = exchange_start(pos, x, ct, own)
        got, keep = lax.optimization_barrier((got, keep))
    pooled = pool_slots(got, tables, maxlen)
    parts = list(pooled[:1])
    for d in range(1, owners):
        back = [(b, a) for a, b in owner_pairs(d, owners)]
        parts.append(lax.ppermute(pooled[d], "tbl", back))
    embedded = place(pos, slot_of_table, parts)
    if tiled:
        embedded, grad_up, grad_down = exchange_end(keep, came, embedded, factor)
    else:
        grad_up, grad_down = grads_plain(x, ct, up, down, factor)
    return embedded, grad_up, grad_down


def by_exchange(owners, groups, wide, rank):
    each, part = wide // groups, rank // owners
    return owners % 2 == 0 and groups % 2 == 0 and each % 16 == 0 and 2 * part % LANES == 0


def solution(mesh):
    rows = P(("grp", "tbl"), None)
    return jax.shard_map(
        on_device,
        mesh=mesh,
        in_specs=(rows, rows, P(), P("tbl", None, None), rows, rows, P(), P()),
        out_specs=(rows, P("tbl", "grp"), P("grp", "tbl")),
        check_vma=False,
    )
```

```python
import functools
import math

import jax
import jax.numpy as jnp
from jax import lax
from jax.experimental import pallas as pl
from jax.experimental.pallas import tpu as pltpu
from jax.sharding import PartitionSpec as P


F32 = jnp.float32
BF16 = jnp.bfloat16
LANES = 128


def room(mebibytes):
    return pltpu.CompilerParams(vmem_limit_bytes=mebibytes * 2**20)


def whole(memory=pltpu.VMEM):
    return pl.BlockSpec(memory_space=memory)


def in_hbm(x):
    return pltpu.with_memory_space_constraint(x, pltpu.HBM)


def owner_at(t, d, owners):
    return 2 * lax.rem((t >> 1) + (d >> 1), owners // 2) + ((t & 1) ^ (d & 1))


def along_z(z, r, far):
    if far & (far - 1) == 0:
        return z ^ r
    return (z + r) % far if isinstance(z, int) else lax.rem(z + r, far)


def owner_pairs(d, owners):
    return [(t, 2 * ((t // 2 + d // 2) % (owners // 2)) + (t % 2 ^ d % 2)) for t in range(owners)]


def masked_ids(slot_ref, ids_ref, lens_ref, maxlen, rows):
    entries, batch = ids_ref.shape
    feats = lens_ref.shape[0]
    slot_of_row = lax.broadcasted_iota(jnp.int32, (entries, feats), 0) // maxlen
    hit = (slot_of_row == slot_ref[...]).astype(F32)
    lens = jnp.dot(hit, lens_ref[...].astype(F32), preferred_element_type=F32)
    place = lax.broadcasted_iota(jnp.int32, (entries, batch), 0) % maxlen
    keep = place.astype(F32) + 0.5 < lens
    return jnp.where(keep, ids_ref[...], rows)


def prep_kernel(pos_ref, *refs, owners, maxlen, rows, chunks):
    sources, mine, rank_ref = refs[:7], refs[7 : 7 + owners], refs[7 + owners]
    targets, masked_ref, sem = refs[8 + owners : 15 + owners], refs[15 + owners], refs[16 + owners]
    slot_ref, ids_ref, lens_ref, x_ref, ct_ref, down_ref, up_ref = targets
    span = x_ref.shape[1] // chunks
    loads = [pltpu.make_async_copy(sources[i], targets[i], sem.at[i]) for i in range(5)]
    weights = []
    for c in range(chunks):
        at = pl.ds(c * span, span)
        for i, part in ((5, (at, slice(None))), (6, (slice(None), at))):
            weights.append(
                pltpu.make_async_copy(sources[i].at[part], targets[i].at[part], sem.at[5 + len(weights)])
            )
    for load in loads + weights:
        load.start()
    for load in loads[:3]:
        load.wait()
    masked_ref[...] = masked_ids(slot_ref, ids_ref, lens_ref, maxlen, rows)
    t = lax.rem(pos_ref[0], owners)
    entries = mine[0].shape[0]
    for d in range(owners):
        start = pl.multiple_of(owner_at(t, d, owners) * entries, maxlen)
        mine[d][...] = masked_ref[pl.ds(start, entries), :]
    for load in loads[3:]:
        load.wait()
    low = dlow = None
    for c in range(chunks):
        at = slice(c * span, (c + 1) * span)
        x = x_ref[:, at]
        dz = (ct_ref[:, at].astype(F32) * x.astype(F32)).astype(BF16)
        weights[2 * c].wait()
        one = jnp.dot(x, down_ref[at, :], preferred_element_type=F32)
        low = one if c == 0 else low + one
        weights[2 * c + 1].wait()
        one = lax.dot_general(
            dz, up_ref[:, at], (((1,), (1,)), ((), ())), preferred_element_type=F32
        )
        dlow = one if c == 0 else dlow + one
    rank_ref[0] = low.astype(BF16)
    rank_ref[1] = dlow.astype(BF16)


def prep(pos, slot_of_table, ids, lengths, x, ct, down, up, owners, maxlen, rows):
    sources = [slot_of_table.reshape(1, -1), ids.T, lengths.T, x, ct, down, up]
    batch, entries = ids.shape
    chunks = 3 if x.shape[1] % (3 * LANES) == 0 else 1
    *mine, rank = pl.pallas_call(
        functools.partial(prep_kernel, owners=owners, maxlen=maxlen, rows=rows, chunks=chunks),
        in_specs=[whole(pltpu.SMEM)] + [whole(pl.ANY)] * 7,
        out_specs=[whole()] * (owners + 1),
        out_shape=[jax.ShapeDtypeStruct((entries // owners, batch), jnp.int32)] * owners
        + [jax.ShapeDtypeStruct((2, batch, down.shape[1]), BF16)],
        scratch_shapes=[pltpu.VMEM(a.shape, a.dtype) for a in sources]
        + [pltpu.VMEM((entries, batch), jnp.int32), pltpu.SemaphoreType.DMA((5 + 2 * chunks,))],
        compiler_params=room(16),
        name="prep",
    )(pos, *[in_hbm(a) for a in sources])
    return mine, rank


def pool_kernel(*refs, groups, maxlen):
    ids_hbm, tables_hbm, outs = refs[:groups], refs[groups], refs[groups + 1 : 2 * groups + 1]
    near, refs = refs[2 * groups + 1 : 3 * groups + 1], refs[3 * groups + 1 :]
    count, batch, width = outs[0].shape
    stage, wide, pooled, sum_ref = refs[0:2], refs[2:4], refs[4:6], refs[6]
    ids_sem, first_sem, table_sem, out_sem = refs[7:]
    rows = stage[0].shape[0]
    firsts = first_sem.shape[0]
    head = rows // firsts
    piece = math.gcd(rows, 48)
    pieces = rows // piece

    def fetch_ids(g, slot):
        start = pl.multiple_of(slot * maxlen, maxlen)
        return pltpu.make_async_copy(ids_hbm[g].at[pl.ds(start, maxlen)], near[g], ids_sem.at[g])

    def fetch_table(slot, at):
        return pltpu.make_async_copy(tables_hbm.at[slot], stage[at], table_sem.at[at])

    def fetch_first(i):
        part = pl.ds(i * head, head)
        return pltpu.make_async_copy(tables_hbm.at[0, part], stage[0].at[part], first_sem.at[i])

    def put(slot, at, g):
        return pltpu.make_async_copy(pooled[at].at[g], outs[g].at[slot], out_sem.at[at * groups + g])

    def widen(at, start, size):
        part = pl.ds(start, size)
        wide[at][part, :] = stage[at][part, :].astype(F32)

    def half(slot, at):
        other = 1 - at

        @pl.when(slot + 1 < count)
        def _():
            fetch_table(slot + 1, other).wait()

        @pl.when(slot + 2 < count)
        def _():
            fetch_table(slot + 2, at).start()

        @pl.when(slot >= 2)
        def _():
            for g in range(groups):
                put(slot - 2, at, g).wait()

        for g in range(groups):
            fetch_ids(g, slot).wait()
            for b in range(batch):
                bag = g * batch + b
                for p in range(bag * pieces // (groups * batch), (bag + 1) * pieces // (groups * batch)):
                    widen(other, p * piece, piece)
                total = wide[at][pl.ds(near[g][0, b], 1), :]
                for k in range(1, maxlen):
                    total = total + wide[at][pl.ds(near[g][k, b], 1), :]
                sum_ref[pl.ds(b, 1), :] = total
            pooled[at][g] = sum_ref[...].astype(BF16)
            put(slot, at, g).start()

            @pl.when(slot + 1 < count)
            def _(g=g):
                fetch_ids(g, slot + 1).start()

    for g in range(groups):
        fetch_ids(g, 0).start()
    for i in range(firsts):
        fetch_first(i).start()
    if count > 1:
        fetch_table(1, 1).start()
    for at in range(2):
        wide[at][pl.ds(rows, 8), :] = jnp.zeros((8, width), F32)
    for i in range(firsts):
        fetch_first(i).wait()
        widen(0, i * head, head)

    def pair(i, carry):
        half(2 * i, 0)

        @pl.when(2 * i + 1 < count)
        def _():
            half(2 * i + 1, 1)

        return carry

    lax.fori_loop(0, (count + 1) // 2, pair, 0)
    for slot in range(max(count - 2, 0), count):
        for g in range(groups):
            put(slot, slot % 2, g).wait()


def pool_slots(ids, tables, maxlen):
    groups, batch = len(ids), ids[0].shape[1]
    slots, rows, width = tables.shape
    firsts = 4 if rows % 64 == 0 else 1
    return pl.pallas_call(
        functools.partial(pool_kernel, groups=groups, maxlen=maxlen),
        in_specs=[whole(pl.ANY)] * (groups + 1),
        out_specs=[whole(pl.ANY)] * groups,
        out_shape=[jax.ShapeDtypeStruct((slots, batch, width), BF16)] * groups,
        scratch_shapes=[pltpu.SMEM((maxlen, batch), jnp.int32)] * groups
        + [pltpu.VMEM((rows, width), BF16)] * 2
        + [pltpu.VMEM((rows + 8, width), F32)] * 2
        + [pltpu.VMEM((groups, batch, width), BF16)] * 2
        + [pltpu.VMEM((batch, width), F32)]
        + [pltpu.SemaphoreType.DMA((n,)) for n in (groups, firsts, 2, 2 * groups)],
        compiler_params=room(16),
        name="pool_slots",
    )(*ids, in_hbm(tables))


def place_kernel(pos_ref, slot_ref, *refs, owners, firsts):
    parts, out_ref, sem = refs[: len(firsts)], refs[-2], refs[-1]
    slots, _, width = parts[0].shape
    t = lax.rem(pos_ref[0], owners)

    def each(act):
        for d, part in zip(firsts, parts):
            first = owner_at(t, d, owners) * slots
            for f in range(slot_ref.shape[0]):
                local = slot_ref[f] - first

                @pl.when((local >= 0) & (local < slots))
                def _(f=f, part=part, local=local):
                    to = out_ref.at[:, pl.ds(f * width, width)]
                    act(pltpu.make_async_copy(part.at[local], to, sem.at[f]))

    each(lambda copy: copy.start())
    each(lambda copy: copy.wait())


def place(pos, slot_of_table, parts, firsts, owners, before=None):
    _, batch, width = parts[0].shape
    feats = slot_of_table.shape[0]
    more = [] if before is None else [before]
    return pl.pallas_call(
        functools.partial(place_kernel, owners=owners, firsts=firsts),
        in_specs=[whole(pltpu.SMEM)] * 2 + [whole(pl.ANY)] * (len(parts) + len(more)),
        out_specs=whole(pl.ANY),
        out_shape=jax.ShapeDtypeStruct((batch, feats * width), BF16),
        input_output_aliases={2 + len(parts): 0} if more else {},
        scratch_shapes=[pltpu.SemaphoreType.DMA((feats,))],
        compiler_params=room(4),
        name="place",
    )(pos, slot_of_table, *parts, *more)


def grads_kernel(pos_ref, own_ref, sib_ref, *refs, owners, groups, chunks):
    tall, far = owners // 2, groups // 2
    sources, keep_ref, sends = refs[:4], refs[4], refs[5 : 4 + 2 * tall]
    both_ref, sum_ref, near_ref, in_sem, sem = refs[4 + 2 * tall : 9 + 2 * tall]
    targets = refs[9 + 2 * tall :]
    g, t = lax.div(pos_ref[0], owners), lax.rem(pos_ref[0], owners)
    core, y, x, z = t & 1, t >> 1, g & 1, g >> 1
    batch, wide = sources[0].shape
    part = own_ref.shape[2] // owners
    pair = 2 * batch
    span = wide // chunks
    loads = []
    for c in range(chunks):
        at = pl.ds(c * span, span)
        loads.append(
            [
                pltpu.make_async_copy(src.at[:, at], dst.at[:, at], in_sem.at[4 * c + i])
                for i, (src, dst) in enumerate(zip(sources, targets))
            ]
        )
        for load in loads[-1]:
            load.start()
    low = jnp.concatenate([own_ref[0], sib_ref[0]], axis=0).astype(F32)
    dlow = jnp.concatenate([own_ref[1], sib_ref[1]], axis=0).astype(F32)
    none = jnp.zeros((pair, part), F32)
    columns = []
    for ry in range(tall):
        owner = 2 * lax.rem(y + ry, tall) + core
        lo, dl = none, none
        for t in range(owners):
            lo = jnp.where(owner == t, low[:, t * part : (t + 1) * part], lo)
            dl = jnp.where(owner == t, dlow[:, t * part : (t + 1) * part], dl)
        columns.append(
            jnp.concatenate(
                [jnp.concatenate([lo, none], axis=1), jnp.concatenate([none, dl], axis=1)], axis=0
            )
        )
    right = jnp.concatenate(columns, axis=1).astype(BF16)
    step = math.gcd(span, 384)
    for c in range(chunks):
        for load in loads[c]:
            load.wait()
        for d in range(c * span, (c + 1) * span, step):
            cols = slice(d, d + step)
            for i in range(2):
                a = targets[2 * i][:, cols]
                dz = targets[2 * i + 1][:, cols].astype(F32) * a.astype(F32)
                both_ref[pl.ds(i * batch, batch), :] = dz.astype(BF16)
                both_ref[pl.ds(pair + i * batch, batch), :] = a
            sum_ref[pl.ds(d, step), :] = lax.dot_general(
                both_ref[...], right, (((0,), (0,)), ((), ())), preferred_element_type=F32
            )
    each = wide // groups
    block = 2 * part
    copies = []
    for i in range(2 * tall - 1, -1, -1):
        rx, ry = i // tall, i % tall
        cols = slice(ry * block, (ry + 1) * block)
        for r in range(far):
            g = 2 * along_z(z, r, far) + (x + rx - 2 * x * rx)
            found = sum_ref[pl.ds(pl.multiple_of(g * each, 16), each), cols]
            if i:
                near_ref[i - 1, r] = found.astype(BF16)
            else:
                keep_ref[r] = found
        if i:
            copies.append(pltpu.make_async_copy(near_ref.at[i - 1], sends[i - 1], sem.at[i - 1]))
            copies[-1].start()
    for copy in copies:
        copy.wait()


def part_grads(pos, own, sib, x, ct, xs, cts, owners, groups):
    batch, wide = x.shape
    rank = own.shape[2]
    tall, far = owners // 2, groups // 2
    block = 2 * (rank // owners)
    shape = (far, wide // groups, block)
    others = 2 * tall - 1
    chunks = 3 if wide % (3 * LANES) == 0 else 1
    step = math.gcd(wide // chunks, 384)
    return pl.pallas_call(
        functools.partial(grads_kernel, owners=owners, groups=groups, chunks=chunks),
        in_specs=[whole(pltpu.SMEM)] + [whole()] * 2 + [whole(pl.ANY)] * 4,
        out_specs=[whole()] + [whole(pltpu.HBM)] * others,
        out_shape=[jax.ShapeDtypeStruct(shape, F32)] + [pltpu.HBM(shape, BF16)] * others,
        scratch_shapes=[
            pltpu.VMEM((4 * batch, step), BF16),
            pltpu.VMEM((wide, tall * block), F32),
            pltpu.VMEM((others, *shape), BF16),
            pltpu.SemaphoreType.DMA((4 * chunks,)),
            pltpu.SemaphoreType.DMA((others,)),
        ]
        + [pltpu.VMEM((batch, wide), BF16)] * 4,
        compiler_params=room(20),
        name="part_grads",
    )(pos, own, sib, in_hbm(x), in_hbm(ct), xs, cts)


def fold_kernel(keep, *refs, far):
    came, outs = refs[:-far], refs[-far:]
    for r in range(far):
        total = keep[r]
        for one in came:
            total = total + one[r].astype(F32)
        outs[r][...] = total.astype(outs[r].dtype)


def fold(keep, came):
    far, rows, block = keep.shape
    return pl.pallas_call(
        functools.partial(fold_kernel, far=far),
        in_specs=[whole()] * (1 + len(came)),
        out_specs=[whole()] * far,
        out_shape=[jax.ShapeDtypeStruct((rows, block), BF16 if r else F32) for r in range(far)],
        compiler_params=room(12),
        name="fold",
    )(keep, *came)


def finish_kernel(*refs, factor):
    up_ref, down_ref = refs[-2:]
    total = refs[0][...]
    for r in refs[1:-2]:
        total = total + r[...].astype(F32)
    total = total * factor
    half = total.shape[1] // 2
    flat = total.T
    up_ref[...] = flat[:half, :]
    down_ref[...] = flat[half:, :]


def finish(keep, came, factor):
    rows, block = keep.shape
    half = block // 2
    shape = jax.ShapeDtypeStruct
    up, down = pl.pallas_call(
        functools.partial(finish_kernel, factor=factor),
        in_specs=[whole()] * (1 + len(came)),
        out_specs=[whole()] * 2,
        out_shape=[shape((half, rows), F32)] * 2,
        compiler_params=room(8),
        name="finish",
    )(keep, *came)
    return up, down.T


def exchange_start(pos, x, ct, own):
    owners, groups = lax.axis_size("tbl"), lax.axis_size("grp")
    tall = owners // 2
    other_core = [(i, i ^ 1) for i in range(owners)]
    xs = lax.ppermute(x, "tbl", other_core)
    cts = lax.ppermute(ct, "tbl", other_core)
    sib = lax.ppermute(own, "tbl", other_core)
    parts = part_grads(pos, own, sib, x, ct, xs, cts, owners, groups)

    def to(rx, ry):
        return [
            (i * owners + j, (i ^ rx) * owners + 2 * ((j // 2 + ry) % tall) + j % 2)
            for i in range(groups)
            for j in range(owners)
        ]

    came = []
    for i in range(1, 2 * tall):
        came.append(lax.ppermute(parts[i], ("grp", "tbl"), to(i // tall, i % tall)))
    return parts[0], came


def exchange_end(keep, came, embedded, factor):
    groups = lax.axis_size("grp")
    far = groups // 2

    def to_z(r):
        return [(i, 2 * along_z(i // 2, r, far) + i % 2) for i in range(groups)]

    out = fold(keep, came)
    last = []
    for r in range(1, far):
        last.append(lax.ppermute(out[r], "grp", to_z(r)))
    embedded, keep = lax.optimization_barrier((embedded, out[0]))
    return embedded, *finish(keep, last, factor)


def grads_plain(x, ct, up, down, factor):
    low = jnp.dot(x, down, preferred_element_type=F32).astype(BF16)
    dz = (ct.astype(F32) * x.astype(F32)).astype(BF16)
    dlow = jnp.dot(dz, up.T, preferred_element_type=F32).astype(BF16)
    part_up = jnp.dot(low.T, dz, preferred_element_type=F32) * factor
    part_down = jnp.dot(x.T, dlow, preferred_element_type=F32) * factor
    owner_up = lax.psum_scatter(part_up, "tbl", scatter_dimension=0, tiled=True)
    owner_down = lax.psum_scatter(part_down, "tbl", scatter_dimension=1, tiled=True)
    return (
        lax.psum_scatter(owner_up, "grp", scatter_dimension=1, tiled=True),
        lax.psum_scatter(owner_down, "grp", scatter_dimension=0, tiled=True),
    )


def on_device(ids, lengths, slot_of_table, tables, x, ct, up, down):
    owners, groups = lax.axis_size("tbl"), lax.axis_size("grp")
    batch = ids.shape[0]
    slots, rows = tables.shape[:2]
    maxlen = ids.shape[1] // (slots * owners)
    factor = 1.0 / math.sqrt(batch * owners * groups)
    tiled = by_exchange(owners, groups, *down.shape)

    pos = lax.axis_index(("grp", "tbl")).astype(jnp.int32).reshape(1)
    mine, own = prep(pos, slot_of_table, ids, lengths, x, ct, down, up, owners, maxlen, rows)
    got = list(mine[:1])
    for d in range(1, owners):
        got.append(lax.ppermute(mine[d], "tbl", owner_pairs(d, owners)))
    if tiled:
        keep, came = exchange_start(pos, x, ct, own)
        got, keep = lax.optimization_barrier((got, keep))
    pooled = pool_slots(got, tables, maxlen)
    parts = list(pooled[:1])
    for d in range(1, owners):
        back = [(b, a) for a, b in owner_pairs(d, owners)]
        parts.append(lax.ppermute(pooled[d], "tbl", back))
    embedded = place(pos, slot_of_table, parts[:-1], range(owners - 1), owners)
    embedded = place(pos, slot_of_table, parts[-1:], (owners - 1,), owners, embedded)
    if tiled:
        embedded, grad_up, grad_down = exchange_end(keep, came, embedded, factor)
    else:
        grad_up, grad_down = grads_plain(x, ct, up, down, factor)
    return embedded, grad_up, grad_down


def by_exchange(owners, groups, wide, rank):
    each, part = wide // groups, rank // owners
    return owners % 2 == 0 and groups % 2 == 0 and each % 16 == 0 and 2 * part % LANES == 0


def solution(mesh):
    rows = P(("grp", "tbl"), None)
    return jax.shard_map(
        on_device,
        mesh=mesh,
        in_specs=(rows, rows, P(), P("tbl", None, None), rows, rows, P(), P()),
        out_specs=(rows, P("tbl", "grp"), P("grp", "tbl")),
        check_vma=False,
    )
```

```python
import functools
import math

import jax
import jax.numpy as jnp
from jax import lax
from jax.experimental import pallas as pl
from jax.experimental.pallas import tpu as pltpu
from jax.sharding import PartitionSpec as P


F32 = jnp.float32
BF16 = jnp.bfloat16
LANES = 128


def room(mebibytes):
    return pltpu.CompilerParams(vmem_limit_bytes=mebibytes * 2**20)


def whole(memory=pltpu.VMEM):
    return pl.BlockSpec(memory_space=memory)


def in_hbm(x):
    return pltpu.with_memory_space_constraint(x, pltpu.HBM)


def owner_at(t, d, owners):
    return 2 * lax.rem((t >> 1) + (d >> 1), owners // 2) + ((t & 1) ^ (d & 1))


def owner_pairs(d, owners):
    return [(t, 2 * ((t // 2 + d // 2) % (owners // 2)) + (t % 2 ^ d % 2)) for t in range(owners)]


def masked_ids(slot_ref, ids_ref, lens_ref, maxlen, rows):
    entries, batch = ids_ref.shape
    feats = lens_ref.shape[0]
    slot_of_row = lax.broadcasted_iota(jnp.int32, (entries, feats), 0) // maxlen
    hit = (slot_of_row == slot_ref[...]).astype(F32)
    lens = jnp.dot(hit, lens_ref[...].astype(F32), preferred_element_type=F32)
    place = lax.broadcasted_iota(jnp.int32, (entries, batch), 0) % maxlen
    keep = place.astype(F32) + 0.5 < lens
    return jnp.where(keep, ids_ref[...], rows)


def prep_kernel(pos_ref, *refs, owners, maxlen, rows):
    sources, mine, rank_ref = refs[:7], refs[7 : 7 + owners], refs[7 + owners]
    targets, masked_ref, sem = refs[8 + owners : 15 + owners], refs[15 + owners], refs[16 + owners]
    slot_ref, ids_ref, lens_ref, x_ref, ct_ref, down_ref, up_ref = targets
    loads = [
        pltpu.make_async_copy(src, dst, sem.at[i]) for i, (src, dst) in enumerate(zip(sources, targets))
    ]
    for load in loads:
        load.start()
    for load in loads[:3]:
        load.wait()
    masked_ref[...] = masked_ids(slot_ref, ids_ref, lens_ref, maxlen, rows)
    t = lax.rem(pos_ref[0], owners)
    entries = mine[0].shape[0]
    for d in range(owners):
        start = pl.multiple_of(owner_at(t, d, owners) * entries, maxlen)
        mine[d][...] = masked_ref[pl.ds(start, entries), :]
    for load in loads[3:5]:
        load.wait()
    x = x_ref[...]
    dz = (ct_ref[...].astype(F32) * x.astype(F32)).astype(BF16)
    loads[5].wait()
    rank_ref[0] = jnp.dot(x, down_ref[...], preferred_element_type=F32).astype(BF16)
    loads[6].wait()
    rank_ref[1] = lax.dot_general(
        dz, up_ref[...], (((1,), (1,)), ((), ())), preferred_element_type=F32
    ).astype(BF16)


def prep(pos, slot_of_table, ids, lengths, x, ct, down, up, owners, maxlen, rows):
    sources = [slot_of_table.reshape(1, -1), ids.T, lengths.T, x, ct, down, up]
    batch, entries = ids.shape
    *mine, rank = pl.pallas_call(
        functools.partial(prep_kernel, owners=owners, maxlen=maxlen, rows=rows),
        in_specs=[whole(pltpu.SMEM)] + [whole(pl.ANY)] * 7,
        out_specs=[whole()] * (owners + 1),
        out_shape=[jax.ShapeDtypeStruct((entries // owners, batch), jnp.int32)] * owners
        + [jax.ShapeDtypeStruct((2, batch, down.shape[1]), BF16)],
        scratch_shapes=[pltpu.VMEM(a.shape, a.dtype) for a in sources]
        + [pltpu.VMEM((entries, batch), jnp.int32), pltpu.SemaphoreType.DMA((7,))],
        compiler_params=room(16),
        name="prep",
    )(pos, *[in_hbm(a) for a in sources])
    return mine, rank


def pool_kernel(*refs, groups, maxlen, ready):
    if ready:
        first_ref, refs = refs[0], refs[1:]
    ids_hbm, tables_hbm, outs = refs[:groups], refs[groups], refs[groups + 1 : 2 * groups + 1]
    near, refs = refs[2 * groups + 1 : 3 * groups + 1], refs[3 * groups + 1 :]
    count, batch, width = outs[0].shape
    stage, wide, pooled, sum_ref = refs[0:2], refs[2:4], refs[4:6], refs[6]
    ids_sem, first_sem, table_sem, out_sem = refs[7:]
    rows = stage[0].shape[0]
    firsts = first_sem.shape[0]
    head = rows // firsts
    piece = math.gcd(rows, 48)
    pieces = rows // piece

    def fetch_ids(g, slot):
        start = pl.multiple_of(slot * maxlen, maxlen)
        return pltpu.make_async_copy(ids_hbm[g].at[pl.ds(start, maxlen)], near[g], ids_sem.at[g])

    def fetch_table(slot, at):
        return pltpu.make_async_copy(tables_hbm.at[slot], stage[at], table_sem.at[at])

    def fetch_first(i):
        part = pl.ds(i * head, head)
        return pltpu.make_async_copy(tables_hbm.at[0, part], stage[0].at[part], first_sem.at[i])

    def put(slot, at, g):
        return pltpu.make_async_copy(pooled[at].at[g], outs[g].at[slot], out_sem.at[at * groups + g])

    def widen(at, start, size):
        part = pl.ds(start, size)
        wide[at][part, :] = stage[at][part, :].astype(F32)

    def half(slot, at):
        other = 1 - at

        @pl.when(slot + 1 < count)
        def _():
            fetch_table(slot + 1, other).wait()

        @pl.when(slot + 2 < count)
        def _():
            fetch_table(slot + 2, at).start()

        @pl.when(slot >= 2)
        def _():
            for g in range(groups):
                put(slot - 2, at, g).wait()

        for g in range(groups):
            fetch_ids(g, slot).wait()
            for b in range(batch):
                bag = g * batch + b
                for p in range(bag * pieces // (groups * batch), (bag + 1) * pieces // (groups * batch)):
                    widen(other, p * piece, piece)
                total = wide[at][pl.ds(near[g][0, b], 1), :]
                for k in range(1, maxlen):
                    total = total + wide[at][pl.ds(near[g][k, b], 1), :]
                sum_ref[pl.ds(b, 1), :] = total
            pooled[at][g] = sum_ref[...].astype(BF16)
            put(slot, at, g).start()

            @pl.when(slot + 1 < count)
            def _(g=g):
                fetch_ids(g, slot + 1).start()

    for g in range(groups):
        fetch_ids(g, 0).start()
    for i in range(0 if ready else firsts):
        fetch_first(i).start()
    if count > 1:
        fetch_table(1, 1).start()
    for at in range(2):
        wide[at][pl.ds(rows, 8), :] = jnp.zeros((8, width), F32)
    for i in range(firsts):
        if ready:
            part = pl.ds(i * head, head)
            wide[0][part, :] = first_ref[part, :].astype(F32)
        else:
            fetch_first(i).wait()
            widen(0, i * head, head)

    def pair(i, carry):
        half(2 * i, 0)

        @pl.when(2 * i + 1 < count)
        def _():
            half(2 * i + 1, 1)

        return carry

    lax.fori_loop(0, (count + 1) // 2, pair, 0)
    for slot in range(max(count - 2, 0), count):
        for g in range(groups):
            put(slot, slot % 2, g).wait()


def pool_slots(ids, tables, maxlen, first=None):
    ready = [] if first is None else [first]
    groups, batch = len(ids), ids[0].shape[1]
    slots, rows, width = tables.shape
    firsts = 4 if rows % 64 == 0 else 1
    return pl.pallas_call(
        functools.partial(pool_kernel, groups=groups, maxlen=maxlen, ready=len(ready) > 0),
        in_specs=[whole()] * len(ready) + [whole(pl.ANY)] * (groups + 1),
        out_specs=[whole(pl.ANY)] * groups,
        out_shape=[jax.ShapeDtypeStruct((slots, batch, width), BF16)] * groups,
        scratch_shapes=[pltpu.SMEM((maxlen, batch), jnp.int32)] * groups
        + [pltpu.VMEM((rows, width), BF16)] * 2
        + [pltpu.VMEM((rows + 8, width), F32)] * 2
        + [pltpu.VMEM((groups, batch, width), BF16)] * 2
        + [pltpu.VMEM((batch, width), F32)]
        + [pltpu.SemaphoreType.DMA((n,)) for n in (groups, firsts, 2, 2 * groups)],
        compiler_params=room(16),
        name="pool_slots",
    )(*ready, *ids, in_hbm(tables))


def place_kernel(pos_ref, slot_ref, *refs):
    parts, out_ref, sem = refs[:-2], refs[-2], refs[-1]
    owners = len(parts)
    slots, _, width = parts[0].shape
    feats = slot_ref.shape[0]
    t = lax.rem(pos_ref[0], owners)

    def put(f, part, local):
        to = out_ref.at[:, pl.ds(f * width, width)]
        return pltpu.make_async_copy(part.at[local], to, sem.at[f])

    for d, part in enumerate(parts):
        first = owner_at(t, d, owners) * slots
        for f in range(feats):
            local = slot_ref[f] - first

            @pl.when((local >= 0) & (local < slots))
            def _(f=f, part=part, local=local):
                put(f, part, local).start()

    for f in range(feats):
        put(f, parts[0], 0).wait()


def place(pos, slot_of_table, parts):
    _, batch, width = parts[0].shape
    feats = slot_of_table.shape[0]
    return pl.pallas_call(
        place_kernel,
        in_specs=[whole(pltpu.SMEM)] * 2 + [whole(pl.ANY)] * len(parts),
        out_specs=whole(pl.ANY),
        out_shape=jax.ShapeDtypeStruct((batch, feats * width), BF16),
        scratch_shapes=[pltpu.SemaphoreType.DMA((feats,))],
        compiler_params=room(4),
        name="place",
    )(pos, slot_of_table, *parts)


def grads_kernel(pos_ref, own_ref, sib_ref, *refs, owners, groups, chunks):
    tall, far = owners // 2, groups // 2
    sources, tables_hbm, keep_ref, sends = refs[:4], refs[4], refs[5], refs[6 : 5 + 2 * tall]
    first_ref, sum_ref, near_ref, in_sem, sem, first_sem = refs[5 + 2 * tall : 11 + 2 * tall]
    targets = refs[11 + 2 * tall :]
    g, t = lax.div(pos_ref[0], owners), lax.rem(pos_ref[0], owners)
    core, y, x, z = t & 1, t >> 1, g & 1, g >> 1
    batch, wide = sources[0].shape
    part = own_ref.shape[2] // owners
    pair = 2 * batch
    span = wide // chunks
    loads = []
    for c in range(chunks):
        at = pl.ds(c * span, span)
        loads.append(
            [
                pltpu.make_async_copy(src.at[:, at], dst.at[:, at], in_sem.at[4 * c + i])
                for i, (src, dst) in enumerate(zip(sources, targets))
            ]
        )
        for load in loads[-1]:
            load.start()
    first = pltpu.make_async_copy(tables_hbm.at[0], first_ref, first_sem)
    first.start()
    low = jnp.concatenate([own_ref[0], sib_ref[0]], axis=0).astype(F32)
    dlow = jnp.concatenate([own_ref[1], sib_ref[1]], axis=0).astype(F32)
    none = jnp.zeros((pair, part), F32)
    columns = []
    for ry in range(tall):
        owner = 2 * lax.rem(y + ry, tall) + core
        lo, dl = none, none
        for t in range(owners):
            lo = jnp.where(owner == t, low[:, t * part : (t + 1) * part], lo)
            dl = jnp.where(owner == t, dlow[:, t * part : (t + 1) * part], dl)
        columns.append(
            jnp.concatenate(
                [jnp.concatenate([lo, none], axis=1), jnp.concatenate([none, dl], axis=1)], axis=0
            )
        )
    right = jnp.concatenate(columns, axis=1).astype(BF16)
    step = math.gcd(span, 384)
    for c in range(chunks):
        for load in loads[c]:
            load.wait()
        for d in range(c * span, (c + 1) * span, step):
            cols = slice(d, d + step)
            xs = [targets[2 * i][:, cols] for i in range(2)]
            dzs = [
                (targets[2 * i + 1][:, cols].astype(F32) * xs[i].astype(F32)).astype(BF16) for i in range(2)
            ]
            sum_ref[pl.ds(d, step), :] = lax.dot_general(
                jnp.concatenate(dzs + xs, axis=0), right, (((0,), (0,)), ((), ())), preferred_element_type=F32
            )
    each = wide // groups
    block = 2 * part
    copies = []
    for i in range(2 * tall - 1, -1, -1):
        rx, ry = i // tall, i % tall
        cols = slice(ry * block, (ry + 1) * block)
        for r in range(far):
            g = 2 * lax.rem(z + r, far) + (x + rx - 2 * x * rx)
            found = sum_ref[pl.ds(pl.multiple_of(g * each, 16), each), cols]
            if i:
                near_ref[i - 1, r] = found.astype(BF16)
            else:
                keep_ref[r] = found
        if i:
            copies.append(pltpu.make_async_copy(near_ref.at[i - 1], sends[i - 1], sem.at[i - 1]))
            copies[-1].start()
    for copy in copies:
        copy.wait()
    first.wait()


def part_grads(pos, own, sib, x, ct, xs, cts, tables, owners, groups):
    batch, wide = x.shape
    rank = own.shape[2]
    tall, far = owners // 2, groups // 2
    block = 2 * (rank // owners)
    shape = (far, wide // groups, block)
    others = 2 * tall - 1
    chunks = 9 if wide % (9 * LANES) == 0 else 1
    return pl.pallas_call(
        functools.partial(grads_kernel, owners=owners, groups=groups, chunks=chunks),
        in_specs=[whole(pltpu.SMEM)] + [whole()] * 2 + [whole(pl.ANY)] * 5,
        out_specs=[whole()] + [whole(pltpu.HBM)] * others + [whole()],
        out_shape=[jax.ShapeDtypeStruct(shape, F32)]
        + [pltpu.HBM(shape, BF16)] * others
        + [jax.ShapeDtypeStruct(tables.shape[1:], BF16)],
        scratch_shapes=[
            pltpu.VMEM((wide, tall * block), F32),
            pltpu.VMEM((others, *shape), BF16),
            pltpu.SemaphoreType.DMA((4 * chunks,)),
            pltpu.SemaphoreType.DMA((others,)),
            pltpu.SemaphoreType.DMA,
        ]
        + [pltpu.VMEM((batch, wide), BF16)] * 4,
        compiler_params=room(20),
        name="part_grads",
    )(pos, own, sib, in_hbm(x), in_hbm(ct), xs, cts, in_hbm(tables))


def fold_kernel(keep, *refs, far):
    came, outs = refs[:-far], refs[-far:]
    for r in range(far):
        total = keep[r]
        for one in came:
            total = total + one[r].astype(F32)
        outs[r][...] = total.astype(outs[r].dtype)


def fold(keep, came):
    far, rows, block = keep.shape
    return pl.pallas_call(
        functools.partial(fold_kernel, far=far),
        in_specs=[whole()] * (1 + len(came)),
        out_specs=[whole()] * far,
        out_shape=[jax.ShapeDtypeStruct((rows, block), BF16 if r else F32) for r in range(far)],
        compiler_params=room(12),
        name="fold",
    )(keep, *came)


def finish_kernel(*refs, factor):
    up_ref, down_ref = refs[-2:]
    total = refs[0][...]
    for r in refs[1:-2]:
        total = total + r[...].astype(F32)
    total = total * factor
    half = total.shape[1] // 2
    flat = total.T
    up_ref[...] = flat[:half, :]
    down_ref[...] = flat[half:, :]


def finish(keep, came, factor):
    rows, block = keep.shape
    half = block // 2
    shape = jax.ShapeDtypeStruct
    up, down = pl.pallas_call(
        functools.partial(finish_kernel, factor=factor),
        in_specs=[whole()] * (1 + len(came)),
        out_specs=[whole()] * 2,
        out_shape=[shape((half, rows), F32)] * 2,
        compiler_params=room(8),
        name="finish",
    )(keep, *came)
    return up, down.T


def exchange_start(pos, x, ct, own, tables):
    owners, groups = lax.axis_size("tbl"), lax.axis_size("grp")
    tall = owners // 2
    other_core = [(i, i ^ 1) for i in range(owners)]
    xs = lax.ppermute(x, "tbl", other_core)
    cts = lax.ppermute(ct, "tbl", other_core)
    sib = lax.ppermute(own, "tbl", other_core)
    *parts, first = part_grads(pos, own, sib, x, ct, xs, cts, tables, owners, groups)

    def to(rx, ry):
        return [
            (i * owners + j, (i ^ rx) * owners + 2 * ((j // 2 + ry) % tall) + j % 2)
            for i in range(groups)
            for j in range(owners)
        ]

    came = []
    for i in range(1, 2 * tall):
        came.append(lax.ppermute(parts[i], ("grp", "tbl"), to(i // tall, i % tall)))
    return parts[0], came, first


def exchange_end(keep, came, embedded, factor):
    groups = lax.axis_size("grp")
    far = groups // 2

    def to_z(r):
        return [(i, 2 * ((i // 2 + r) % far) + i % 2) for i in range(groups)]

    out = fold(keep, came)
    last = []
    for r in range(1, far):
        last.append(lax.ppermute(out[r], "grp", to_z(r)))
    embedded, keep = lax.optimization_barrier((embedded, out[0]))
    return embedded, *finish(keep, last, factor)


def grads_plain(x, ct, up, down, factor):
    low = jnp.dot(x, down, preferred_element_type=F32).astype(BF16)
    dz = (ct.astype(F32) * x.astype(F32)).astype(BF16)
    dlow = jnp.dot(dz, up.T, preferred_element_type=F32).astype(BF16)
    part_up = jnp.dot(low.T, dz, preferred_element_type=F32) * factor
    part_down = jnp.dot(x.T, dlow, preferred_element_type=F32) * factor
    owner_up = lax.psum_scatter(part_up, "tbl", scatter_dimension=0, tiled=True)
    owner_down = lax.psum_scatter(part_down, "tbl", scatter_dimension=1, tiled=True)
    return (
        lax.psum_scatter(owner_up, "grp", scatter_dimension=1, tiled=True),
        lax.psum_scatter(owner_down, "grp", scatter_dimension=0, tiled=True),
    )


def on_device(ids, lengths, slot_of_table, tables, x, ct, up, down):
    owners, groups = lax.axis_size("tbl"), lax.axis_size("grp")
    batch = ids.shape[0]
    slots, rows = tables.shape[:2]
    maxlen = ids.shape[1] // (slots * owners)
    factor = 1.0 / math.sqrt(batch * owners * groups)
    tiled = by_exchange(owners, groups, *down.shape)

    pos = lax.axis_index(("grp", "tbl")).astype(jnp.int32).reshape(1)
    mine, own = prep(pos, slot_of_table, ids, lengths, x, ct, down, up, owners, maxlen, rows)
    got = list(mine[:1])
    for d in range(1, owners):
        got.append(lax.ppermute(mine[d], "tbl", owner_pairs(d, owners)))
    first = None
    if tiled:
        keep, came, first = exchange_start(pos, x, ct, own, tables)
        got, keep = lax.optimization_barrier((got, keep))
    pooled = pool_slots(got, tables, maxlen, first)
    parts = list(pooled[:1])
    for d in range(1, owners):
        back = [(b, a) for a, b in owner_pairs(d, owners)]
        parts.append(lax.ppermute(pooled[d], "tbl", back))
    embedded = place(pos, slot_of_table, parts)
    if tiled:
        embedded, grad_up, grad_down = exchange_end(keep, came, embedded, factor)
    else:
        grad_up, grad_down = grads_plain(x, ct, up, down, factor)
    return embedded, grad_up, grad_down


def by_exchange(owners, groups, wide, rank):
    each, part = wide // groups, rank // owners
    return owners % 2 == 0 and groups % 2 == 0 and each % 16 == 0 and 2 * part % LANES == 0


def solution(mesh):
    rows = P(("grp", "tbl"), None)
    return jax.shard_map(
        on_device,
        mesh=mesh,
        in_specs=(rows, rows, P(), P("tbl", None, None), rows, rows, P(), P()),
        out_specs=(rows, P("tbl", "grp"), P("grp", "tbl")),
        check_vma=False,
    )
```
